32 devices in a mesh: data: 32 (over z, y, x, core).
Axes of the slice: x: 2, y: 2, z: 4, core: 2. Of those that a mesh axis runs over, the one named last changes fastest.
Arguments:
- w_in: float32 [4096, 512], replicated
- w_up: float32 [12, 512, 2048], replicated
- w_down: float32 [12, 2048, 512], replicated
- mom_in: float32 [4096, 512], replicated
- mom_up: float32 [12, 512, 2048], replicated
- mom_down: float32 [12, 2048, 512], replicated
- x_now: bfloat16 [8192, 4096], P('data')
- y_now: bfloat16 [8192, 512], P('data')
- x_next: bfloat16 [8192, 4096], P('data')
- y_next: bfloat16 [8192, 512], P('data')
Outputs:
- output 1: float32 [4096, 512], replicated
- output 2: float32 [12, 512, 2048], replicated
- output 3: float32 [12, 2048, 512], replicated
- output 4: float32 [4096, 512], replicated
- output 5: float32 [12, 512, 2048], replicated
- output 6: float32 [12, 2048, 512], replicated
- output 7: float32 [8192], P('data')
- output 8: float32 [8192, 512], P('data')
All inputs are finite; a program needn't handle non-finite values.
Results may differ from the reference program's by a relative error of at most 0.0119842.
Values are sent between devices in bfloat16 or wider.
A program may use at most 1.75 GiB of HBM per device.

```python
import jax
import jax.numpy as jnp
from jax import lax

D = 512
FF = 2048
E = 4096
LAYERS = 12
BATCH_ROWS = 8192
STEP_SIZE = 4.0 * D / (FF * (LAYERS + 1))
MOMENTUM = 0.9


def setup_inputs(seed: int = 0) -> dict:
    key_list = jax.random.split(jax.random.key(seed), 10)
    in_scale = E ** -0.5
    up_scale = D ** -0.5
    down_scale = (FF * LAYERS) ** -0.5
    mom_factor = 0.75 / D
    return {
        "w_in": jax.random.normal(key_list[0], (E, D), jnp.float32) * in_scale,
        "w_up": jax.random.normal(key_list[1], (LAYERS, D, FF), jnp.float32) * up_scale,
        "w_down": jax.random.normal(key_list[2], (LAYERS, FF, D), jnp.float32) * down_scale,
        "mom_in": jax.random.normal(key_list[3], (E, D), jnp.float32) * (in_scale * mom_factor),
        "mom_up": jax.random.normal(key_list[4], (LAYERS, D, FF), jnp.float32) * (up_scale * mom_factor),
        "mom_down": jax.random.normal(key_list[5], (LAYERS, FF, D), jnp.float32) * (down_scale * mom_factor),
        "x_now": jax.random.normal(key_list[6], (BATCH_ROWS, E), jnp.float32).astype(jnp.bfloat16),
        "y_now": jax.random.normal(key_list[7], (BATCH_ROWS, D), jnp.float32).astype(jnp.bfloat16),
        "x_next": jax.random.normal(key_list[8], (BATCH_ROWS, E), jnp.float32).astype(jnp.bfloat16),
        "y_next": jax.random.normal(key_list[9], (BATCH_ROWS, D), jnp.float32).astype(jnp.bfloat16),
    }


def gelu_tanh(pre_value):
    return jax.nn.gelu(pre_value, approximate=True)


def stack_forward(w_in, w_up, w_down, x_rows):
    h_first = jnp.dot(x_rows, w_in.astype(jnp.bfloat16), preferred_element_type=jnp.float32)

    def layer_step(h_state, layer_weights):
        up_mat, down_mat = layer_weights
        h_low = h_state.astype(jnp.bfloat16)
        pre_act = jnp.dot(h_low, up_mat.astype(jnp.bfloat16), preferred_element_type=jnp.float32)
        act_low = gelu_tanh(pre_act).astype(jnp.bfloat16)
        h_state = h_state + jnp.dot(act_low, down_mat.astype(jnp.bfloat16), preferred_element_type=jnp.float32)
        return h_state, h_low

    return lax.scan(layer_step, h_first, (w_up, w_down))


def stack_gradients(w_in, w_up, w_down, x_rows, y_rows):
    h_last, layer_inputs = stack_forward(w_in, w_up, w_down, x_rows)
    cot_last = (h_last - y_rows.astype(jnp.float32)) / (BATCH_ROWS * D)

    def layer_back(cot_state, packed):
        up_mat, down_mat, h_low = packed
        up_low = up_mat.astype(jnp.bfloat16)
        down_low = down_mat.astype(jnp.bfloat16)
        pre_act = jnp.dot(h_low, up_low, preferred_element_type=jnp.float32)
        act_val, gelu_back = jax.vjp(gelu_tanh, pre_act)
        act_low = act_val.astype(jnp.bfloat16)
        cot_low = cot_state.astype(jnp.bfloat16)
        grad_down = jnp.dot(act_low.T, cot_low, preferred_element_type=jnp.float32)
        act_cot = jnp.dot(cot_low, down_low.T, preferred_element_type=jnp.float32)
        pre_cot = gelu_back(act_cot)[0].astype(jnp.bfloat16)
        grad_up = jnp.dot(h_low.T, pre_cot, preferred_element_type=jnp.float32)
        cot_state = cot_state + jnp.dot(pre_cot, up_low.T, preferred_element_type=jnp.float32)
        return cot_state, (grad_up, grad_down)

    cot_first, layer_grads = lax.scan(layer_back, cot_last, (w_up, w_down, layer_inputs), reverse=True)
    grad_in = jnp.dot(x_rows.T, cot_first.astype(jnp.bfloat16), preferred_element_type=jnp.float32)
    return grad_in, layer_grads[0], layer_grads[1]


def reference(w_in, w_up, w_down, mom_in, mom_up, mom_down, x_now, y_now, x_next, y_next):
    grad_in, grad_up, grad_down = stack_gradients(w_in, w_up, w_down, x_now, y_now)
    new_mom_in = MOMENTUM * mom_in + grad_in
    new_mom_up = MOMENTUM * mom_up + grad_up
    new_mom_down = MOMENTUM * mom_down + grad_down
    new_w_in = w_in - STEP_SIZE * new_mom_in
    new_w_up = w_up - STEP_SIZE * new_mom_up
    new_w_down = w_down - STEP_SIZE * new_mom_down
    h_next = stack_forward(new_w_in, new_w_up, new_w_down, x_next)[0]
    loss_next = jnp.sum(jnp.square(h_next - y_next.astype(jnp.float32)), axis=1) / (2 * D)
    return (new_w_in, new_w_up, new_w_down, new_mom_in, new_mom_up, new_mom_down, loss_next, h_next)
```

```python
import functools

import jax
import jax.numpy as jnp
from jax import lax
from jax.experimental import pallas as pl
from jax.experimental.pallas import tpu as pltpu
from jax.sharding import PartitionSpec as P

MOMENTUM = 0.9
MESH = pl.DeviceIdType.MESH
BIT = {"c": 1, "x": 2, "y": 4, "a": 8, "b": 16}

def ar_kernel(nu, tr, tw, lags, orders, *refs):
    (g, gs, acc, fin, rb0, rb1, rb2, rb3, rb4, ld_s, c_s, c_r, rs_s, rs_r, ag_s, ag_r, d_s, d_r, st_s) = refs
    K = ld_s.shape[0]
    NS, NF = acc.shape[0], fin.shape[0]
    l0, lrs, lag_, ld = lags
    me = lax.axis_index("data")
    bit = {d: lax.rem(me // BIT[d], 2) for d in BIT}
    peer = {d: me + BIT[d] * (1 - 2 * bit[d]) for d in BIT}
    bar = pltpu.get_barrier_semaphore()
    for d in "cxyab":
        pl.semaphore_signal(bar, inc=1, device_id=(peer[d],), device_id_type=MESH)
    pl.semaphore_wait(bar, 5)
    half = tr // 2
    rbs = [None, rb1, rb2, rb3, rb4]
    base, size = [], [half >> s for s in range(5)]
    for k, od in enumerate(orders):
        b = [k * half]
        for s, d in enumerate(od):
            b.append(b[-1] + size[s + 1] * bit[d])
        base.append(b)
    give = [[base[k][s] + size[s + 1] * (1 - bit[d]) for s, d in enumerate(od)] for k, od in enumerate(orders)]
    o = [0, l0]
    for s in range(4): o.append(o[-1] + lrs[s])
    for s in range(4): o.append(o[-1] + lag_[s])
    o.append(o[-1] + ld)
    assert NS >= o[5] and NF >= o[10] - o[1]
    AL = min(16, half // 16)
    def rows(off, n):
        return pl.ds(pl.multiple_of(off, AL), n)
    def cp_load(u):
        return pltpu.make_async_copy(g.at[u, bit["c"]], acc.at[lax.rem(u, NS)], ld_s.at[lax.rem(u, K)])
    def cp_c(u):
        return pltpu.make_async_remote_copy(src_ref=g.at[u, 1 - bit["c"]], dst_ref=rb0.at[lax.rem(u, K)],
            send_sem=c_s.at[lax.rem(u, K)], recv_sem=c_r.at[lax.rem(u, K)], device_id=(peer["c"],), device_id_type=MESH)
    def cp_rs(u, k, s):
        return pltpu.make_async_remote_copy(src_ref=acc.at[lax.rem(u, NS), rows(give[k][s - 1], size[s])], dst_ref=rbs[s].at[k, lax.rem(u, K)],
            send_sem=rs_s.at[s - 1, k, lax.rem(u, K)], recv_sem=rs_r.at[s - 1, k, lax.rem(u, K)],
            device_id=(peer[orders[k][s - 1]],), device_id_type=MESH)
    def cp_ag(u, k, s):
        sl = fin.at[lax.rem(u, NF), rows(base[k][s], size[s])]
        return pltpu.make_async_remote_copy(src_ref=sl, dst_ref=sl, send_sem=ag_s.at[s - 1, k, lax.rem(u, K)], recv_sem=ag_r.at[s - 1, k, lax.rem(u, K)],
            device_id=(peer[orders[k][s - 1]],), device_id_type=MESH)
    def cp_d(u):
        return pltpu.make_async_remote_copy(src_ref=fin.at[lax.rem(u, NF)], dst_ref=gs.at[u, bit["c"]],
            send_sem=d_s.at[lax.rem(u, K)], recv_sem=d_r.at[lax.rem(u, K)], device_id=(peer["c"],), device_id_type=MESH)
    def cp_st(u):
        return pltpu.make_async_copy(fin.at[lax.rem(u, NF)], gs.at[u, bit["c"]], st_s.at[lax.rem(u, K)])
    def add_c(u):
        sl = lax.rem(u, NS)
        for h in range(4):
            r = slice(h * tr // 4, (h + 1) * tr // 4)
            acc[sl, r] = (acc[sl, r].astype(jnp.float32) + rb0[lax.rem(u, K), r].astype(jnp.float32)).astype(jnp.bfloat16)
    def add_rs(u, k, s):
        sl = lax.rem(u, NS)
        r = rows(base[k][s], size[s])
        out, so = (fin, lax.rem(u, NF)) if s == 4 else (acc, sl)
        out[so, r] = (acc[sl, r].astype(jnp.float32) + rbs[s][k, lax.rem(u, K)].astype(jnp.float32)).astype(jnp.bfloat16)

    def tick(t, _):
        def ev(e, f):
            u = t - o[e]
            @pl.when(jnp.logical_and(u >= 0, u < nu))
            def _():
                f(u)
        def e10(u):
            cp_d(u).wait(); cp_st(u).wait()
        def e9(u):
            for k in range(2): cp_ag(u, k, 1).wait()
            cp_d(u).start(); cp_st(u).start()
        def mk_ag(s):
            def f(u):
                for k in range(2): cp_ag(u, k, s).wait()
                for k in range(2): cp_ag(u, k, s - 1).start()
            return f
        def e5(u):
            for k in range(2):
                cp_rs(u, k, 4).wait(); add_rs(u, k, 4)
            for k in range(2): cp_ag(u, k, 4).start()
        def mk_rs(s):
            def f(u):
                for k in range(2):
                    cp_rs(u, k, s - 1).wait(); add_rs(u, k, s - 1)
                for k in range(2): cp_rs(u, k, s).start()
            return f
        def e1(u):
            cp_load(u).wait(); cp_c(u).wait(); add_c(u)
            for k in range(2): cp_rs(u, k, 1).start()
        def e0(u):
            cp_load(u).start(); cp_c(u).start()
        ev(10, e10); ev(9, e9)
        for e, s in ((8, 2), (7, 3), (6, 4)): ev(e, mk_ag(s))
        ev(5, e5)
        for e in (4, 3, 2): ev(e, mk_rs(e))
        ev(1, e1); ev(0, e0)
        return 0
    lax.fori_loop(0, nu + o[10], tick, 0)

def all_reduce(g, lags=(1, (2, 2, 2, 2), (2, 2, 2, 2), 1), orders=("xayb", "yaxb"), cid=0):
    nu, _, tr, tw = g.shape
    l0, lrs, lag_, ld = lags
    K = 2 * max(l0, ld, *lrs, *lag_)
    NS = l0 + sum(lrs)
    NF = sum(lrs) + sum(lag_) + ld
    bf = jnp.bfloat16
    half = tr // 2
    return pl.pallas_call(
        functools.partial(ar_kernel, nu, tr, tw, lags, orders),
        out_shape=jax.ShapeDtypeStruct(g.shape, bf),
        in_specs=[pl.BlockSpec(memory_space=pl.ANY)],
        out_specs=pl.BlockSpec(memory_space=pl.ANY),
        scratch_shapes=[pltpu.VMEM((NS, tr, tw), bf), pltpu.VMEM((NF, tr, tw), bf), pltpu.VMEM((K, tr, tw), bf)]
        + [pltpu.VMEM((2, K, half >> s, tw), bf) for s in range(1, 5)]
        + [pltpu.SemaphoreType.DMA((K,))] * 3 + [pltpu.SemaphoreType.DMA((4, 2, K))] * 4 + [pltpu.SemaphoreType.DMA((K,))] * 3,
        compiler_params=pltpu.CompilerParams(collective_id=cid, has_side_effects=True, vmem_limit_bytes=56 * 2**20),
        name="grad_sum",
    )(g)

bf, f32 = jnp.bfloat16, jnp.float32
TN = (((0,), (0,)), ((), ()))
NT = (((1,), (1,)), ((), ()))
def dot(a, b): return jnp.dot(a, b, preferred_element_type=f32)
def gelu_tanh(v): return jax.nn.gelu(v, approximate=True)

def fwd_kernel(layers, x, w_in, w_up, w_down, p_out, h_out, h):
    i = pl.program_id(0)
    @pl.when(i < 4)
    def _():
        kq = x.shape[1]
        part = dot(x[...], w_in[...].astype(bf))
        @pl.when(i == 0)
        def _(): h[...] = part
        @pl.when(i > 0)
        def _(): h[...] += part
    @pl.when(i >= 4)
    def _():
        p = h[...].astype(bf)
        p_out[0] = p
        n = w_up.shape[2] // 4
        for q in range(4):
            c = slice(q * n, (q + 1) * n)
            u = dot(p, w_up[0, :, c].astype(bf))
            a = gelu_tanh(u).astype(bf)
            h[...] += dot(a, w_down[0, c, :].astype(bf))
    @pl.when(i == layers + 3)
    def _(): h_out[...] = h[...]

def forward(x, w_in, w_up, w_down):
    rows, e = x.shape
    layers, d, ff = w_up.shape
    lay = lambda i: jnp.maximum(i - 4, 0)
    return pl.pallas_call(
        functools.partial(fwd_kernel, layers), grid=(layers + 4,),
        out_shape=[jax.ShapeDtypeStruct((layers, rows, d), bf), jax.ShapeDtypeStruct((rows, d), f32)],
        in_specs=[pl.BlockSpec((rows, e // 4), lambda i: (0, jnp.minimum(i, 3))), pl.BlockSpec((e // 4, d), lambda i: (jnp.minimum(i, 3), 0)),
                  pl.BlockSpec((1, d, ff), lambda i: (lay(i), 0, 0)), pl.BlockSpec((1, ff, d), lambda i: (lay(i), 0, 0))],
        out_specs=[pl.BlockSpec((1, rows, d), lambda i: (lay(i), 0, 0)), pl.BlockSpec((rows, d), lambda i: (0, 0))],
        scratch_shapes=[pltpu.VMEM((rows, d), f32)],
        compiler_params=pltpu.CompilerParams(vmem_limit_bytes=60 * 2**20), name="forward",
    )(x, w_in, w_up, w_down)

def bwd_kernel(layers, scale, x, y, h_last, p, w_up, w_down, g, c_state):
    i = pl.program_id(0)
    d, ff = w_up.shape[1:]
    @pl.when(i == 0)
    def _(): c_state[...] = (h_last[...] - y[...].astype(f32)) / scale
    @pl.when(i < layers)
    def _():
        c_low = c_state[...].astype(bf)
        pl_ = p[0]
        n = ff // 4
        for q in range(4):
            c = slice(q * n, (q + 1) * n)
            wu = w_up[0, :, c].astype(bf)
            u = dot(pl_, wu)
            act, back = jax.vjp(gelu_tanh, u)
            a = act.astype(bf)
            ac = lax.dot_general(c_low, w_down[0, c, :].astype(bf), NT, preferred_element_type=f32)
            pre = back(ac)[0].astype(bf)
            gd = lax.dot_general(a, c_low, TN, preferred_element_type=f32).astype(bf)
            gu = lax.dot_general(pl_, pre, TN, preferred_element_type=f32).astype(bf)
            g[q, 0] = gu[:, :n // 2]
            g[q, 1] = gu[:, n // 2:]
            for j in range(2):
                g[4 + 2 * (q // 2) + j, q % 2] = gd[:, j * (d // 2):(j + 1) * (d // 2)]
            c_state[...] += lax.dot_general(pre, wu, NT, preferred_element_type=f32)
    @pl.when(i == layers)
    def _():
        c_low = c_state[...].astype(bf)
        for q in range(8):
            gi = lax.dot_general(x[:, q * 512:(q + 1) * 512], c_low, TN, preferred_element_type=f32).astype(bf)
            for j in range(2):
                g[2 * (q // 2) + j, q % 2] = gi[:, j * (d // 2):(j + 1) * (d // 2)]

def backward(scale, x, y, h_last, p, w_up, w_down):
    rows, e = x.shape
    layers, d, ff = w_up.shape
    lay = lambda i: jnp.maximum(layers - 1 - i, 0)
    nu = 8 * (layers + 1)
    return pl.pallas_call(
        functools.partial(bwd_kernel, layers, scale), grid=(layers + 1,),
        out_shape=jax.ShapeDtypeStruct((nu, 2, 512, d // 2), bf),
        in_specs=[pl.BlockSpec((rows, e), lambda i: (0, 0)), pl.BlockSpec((rows, d), lambda i: (0, 0)), pl.BlockSpec((rows, d), lambda i: (0, 0)),
                  pl.BlockSpec((1, rows, d), lambda i: (lay(i), 0, 0)),
                  pl.BlockSpec((1, d, ff), lambda i: (lay(i), 0, 0)), pl.BlockSpec((1, ff, d), lambda i: (lay(i), 0, 0))],
        out_specs=pl.BlockSpec((8, 2, 512, d // 2), lambda i: (layers - i, 0, 0, 0)),
        scratch_shapes=[pltpu.VMEM((rows, d), f32)],
        compiler_params=pltpu.CompilerParams(vmem_limit_bytes=60 * 2**20), name="backward",
    )(x, y, h_last, p, w_up, w_down)

def upd_kernel(layers, eta, mu, x, y, g, w_in, w_up, w_down, m_in, m_up, m_down,
               nw_in, nw_up, nw_down, nm_in, nm_up, nm_down, loss, h_out, h, p, a):
    i = pl.program_id(0)
    d = h.shape[1]
    d2 = d // 2
    v = i - 8
    r = lax.rem(jnp.maximum(v, 0), 8)
    def upd(w, m, nw, nm, t, ix):
        nmv = mu * m[ix] + g[0, t].astype(f32)
        nm[ix] = nmv
        nwv = w[ix] - eta * nmv
        nw[ix] = nwv
        return nwv.astype(bf)
    @pl.when(i < 8)
    def _():
        j = lax.rem(i, 2)
        cols = pl.ds(pl.multiple_of(j * d2, d2), d2)
        tot = None
        for t in range(2):
            s = slice(512 * t, 512 * (t + 1))
            wl = upd(w_in, m_in, nw_in, nm_in, t, (s, slice(None)))
            q = dot(x[:, s], wl)
            tot = q if tot is None else tot + q
        @pl.when(i < 2)
        def _(): h[:, cols] = tot
        @pl.when(i >= 2)
        def _(): h[:, cols] += tot
    @pl.when(jnp.logical_and(v >= 0, r == 0))
    def _(): p[...] = h[...].astype(bf)
    @pl.when(jnp.logical_and(v >= 0, r < 4))
    def _():
        for t in range(2):
            s = slice(d2 * t, d2 * (t + 1))
            wl = upd(w_up, m_up, nw_up, nm_up, t, (0, slice(None), s))
            u = dot(p[...], wl)
            a[r, :, s] = gelu_tanh(u).astype(bf)
    @pl.when(jnp.logical_and(v >= 0, r >= 4))
    def _():
        j = lax.rem(r, 2)
        ig = (r - 4) // 2
        cols = pl.ds(pl.multiple_of(j * d2, d2), d2)
        tot = None
        for t in range(2):
            s = slice(512 * t, 512 * (t + 1))
            wl = upd(w_down, m_down, nw_down, nm_down, t, (0, s, slice(None)))
            q = dot(a[2 * ig + t], wl)
            tot = q if tot is None else tot + q
        h[:, cols] += tot
    @pl.when(i == 8 * layers + 7)
    def _():
        h_out[...] = h[...]
        e = h[...] - y[...].astype(f32)
        loss[...] = jnp.sum(e * e, axis=1, keepdims=True) / (2 * d)

def update(eta, mu, x, y, g, w_in, w_up, w_down, m_in, m_up, m_down):
    rows, e = x.shape
    layers, d, ff = w_up.shape
    nu = 8 * (layers + 1)
    def ii(i):
        u = jnp.minimum(i, 7); return (u // 2, lax.rem(u, 2))
    def iu(i):
        v = jnp.maximum(i - 8, 0); return (v // 8, 0, jnp.minimum(lax.rem(v, 8), 3))
    def idn(i):
        v = jnp.maximum(i - 8, 0); q = jnp.maximum(lax.rem(v, 8) - 4, 0); return (v // 8, q // 2, lax.rem(q, 2))
    s_in = pl.BlockSpec((1024, d // 2), ii)
    s_up = pl.BlockSpec((1, d, 512), iu)
    s_dn = pl.BlockSpec((1, 1024, d // 2), idn)
    x_spec = pl.BlockSpec((rows, 1024), lambda i: (0, jnp.minimum(i, 7) // 2))
    full = pl.BlockSpec((rows, d), lambda i: (0, 0))
    o = [jax.ShapeDtypeStruct(t.shape, f32) for t in (w_in, w_up, w_down, m_in, m_up, m_down)]
    o += [jax.ShapeDtypeStruct((rows, 1), f32), jax.ShapeDtypeStruct((rows, d), f32)]
    return pl.pallas_call(
        functools.partial(upd_kernel, layers, eta, mu), grid=(nu,), out_shape=o,
        in_specs=[x_spec, full, pl.BlockSpec((1, 2, 512, d // 2), lambda i: (i, 0, 0, 0)), s_in, s_up, s_dn, s_in, s_up, s_dn],
        out_specs=[s_in, s_up, s_dn, s_in, s_up, s_dn, pl.BlockSpec((rows, 1), lambda i: (0, 0)), full],
        scratch_shapes=[pltpu.VMEM((rows, d), f32), pltpu.VMEM((rows, d), bf), pltpu.VMEM((4, rows, 512), bf)],
        compiler_params=pltpu.CompilerParams(vmem_limit_bytes=60 * 2**20), name="update",
    )(x, y, g, w_in, w_up, w_down, m_in, m_up, m_down)


def solution(mesh):
    group_size = mesh.shape["data"]

    def device_steps(w_in, w_up, w_down, mom_in, mom_up, mom_down, x_now, y_now, x_next, y_next):
        local_rows, model_width = y_now.shape
        step_size = 4.0 * model_width / (w_up.shape[2] * (w_up.shape[0] + 1))
        p_all, h_last = forward(x_now, w_in, w_up, w_down)
        local = backward(float(local_rows * group_size * model_width), x_now, y_now, h_last, p_all, w_up, w_down)
        total = all_reduce(local, lags=(1, (3, 3, 3, 3), (3, 3, 3, 3), 1))
        out = update(step_size, MOMENTUM, x_next, y_next, total, w_in, w_up, w_down, mom_in, mom_up, mom_down)
        return (*out[:6], out[6][:, 0], out[7])

    row_spec = P("data", None)
    return jax.shard_map(
        device_steps,
        mesh=mesh,
        in_specs=(P(),) * 6 + (row_spec,) * 4,
        out_specs=(P(),) * 6 + (P("data"), row_spec),
        check_vma=False,
    )
```

```python
import functools

import jax
import jax.numpy as jnp
from jax import lax
from jax.experimental import pallas as pl
from jax.experimental.pallas import tpu as pltpu
from jax.sharding import PartitionSpec as P

MOMENTUM = 0.9
MESH = pl.DeviceIdType.MESH
BIT = {"c": 1, "x": 2, "y": 4, "a": 8, "b": 16}

bf, f32 = jnp.bfloat16, jnp.float32
TN = (((0,), (0,)), ((), ()))
NT = (((1,), (1,)), ((), ()))
def dot(a, b): return jnp.dot(a, b, preferred_element_type=f32)
def gelu_tanh(v): return jax.nn.gelu(v, approximate=True)

def back_sum_kernel(layers, scale, nu, tr, tw, lags, orders, *refs):
    (x, y, h_last, p_all, w_up, w_dn, gs, c_state, c_low, wup, wdn, w_s, g, acc, fin, rb0, rb1, rb2, rb3, rb4, c_s, c_r, rs_s, rs_r, ag_s, ag_r, d_s, d_r, st_s) = refs
    K = c_s.shape[0]
    NS, NF = acc.shape[0], fin.shape[0]
    l0, lrs, lag_, ld = lags
    me = lax.axis_index("data")
    bit = {d: lax.rem(me // BIT[d], 2) for d in BIT}
    peer = {d: me + BIT[d] * (1 - 2 * bit[d]) for d in BIT}
    bar = pltpu.get_barrier_semaphore()
    for d in "cxyab":
        pl.semaphore_signal(bar, inc=1, device_id=(peer[d],), device_id_type=MESH)
    pl.semaphore_wait(bar, 5)
    half = tr // 2
    rbs = [None, rb1, rb2, rb3, rb4]
    base, size = [], [half >> s for s in range(5)]
    for k, od in enumerate(orders):
        b = [k * half]
        for s, d in enumerate(od):
            b.append(b[-1] + size[s + 1] * bit[d])
        base.append(b)
    give = [[base[k][s] + size[s + 1] * (1 - bit[d]) for s, d in enumerate(od)] for k, od in enumerate(orders)]
    o = [0, l0]
    for s in range(4): o.append(o[-1] + lrs[s])
    for s in range(4): o.append(o[-1] + lag_[s])
    o.append(o[-1] + ld)
    assert NS >= o[5] and NF >= o[10] - o[1]
    AL = min(16, half // 16)
    def rows(off, n):
        return pl.ds(pl.multiple_of(off, AL), n)
    def own(u): return lax.rem(u // 8, 2), lax.rem(u, 8)
    def out(u): return nu - 8 - 8 * (u // 8) + lax.rem(u, 8)
    def cp_c(u):
        return pltpu.make_async_remote_copy(src_ref=g.at[(*own(u), 1 - bit["c"])], dst_ref=rb0.at[lax.rem(u, K)],
            send_sem=c_s.at[lax.rem(u, K)], recv_sem=c_r.at[lax.rem(u, K)], device_id=(peer["c"],), device_id_type=MESH)
    def cp_rs(u, k, s):
        return pltpu.make_async_remote_copy(src_ref=acc.at[lax.rem(u, NS), rows(give[k][s - 1], size[s])], dst_ref=rbs[s].at[k, lax.rem(u, K)],
            send_sem=rs_s.at[s - 1, k, lax.rem(u, K)], recv_sem=rs_r.at[s - 1, k, lax.rem(u, K)],
            device_id=(peer[orders[k][s - 1]],), device_id_type=MESH)
    def cp_ag(u, k, s):
        sl = fin.at[lax.rem(u, NF), rows(base[k][s], size[s])]
        return pltpu.make_async_remote_copy(src_ref=sl, dst_ref=sl, send_sem=ag_s.at[s - 1, k, lax.rem(u, K)], recv_sem=ag_r.at[s - 1, k, lax.rem(u, K)],
            device_id=(peer[orders[k][s - 1]],), device_id_type=MESH)
    def cp_d(u):
        return pltpu.make_async_remote_copy(src_ref=fin.at[lax.rem(u, NF)], dst_ref=gs.at[out(u), bit["c"]],
            send_sem=d_s.at[lax.rem(u, K)], recv_sem=d_r.at[lax.rem(u, K)], device_id=(peer["c"],), device_id_type=MESH)
    def cp_st(u):
        return pltpu.make_async_copy(fin.at[lax.rem(u, NF)], gs.at[out(u), bit["c"]], st_s.at[lax.rem(u, K)])
    def add_c(u):
        sl = lax.rem(u, NS)
        so, uo = own(u)
        for h in range(4):
            r = slice(h * tr // 4, (h + 1) * tr // 4)
            acc[sl, r] = (g[so, uo, bit["c"], r].astype(f32) + rb0[lax.rem(u, K), r].astype(f32)).astype(bf)
    def add_rs(u, k, s):
        sl = lax.rem(u, NS)
        r = rows(base[k][s], size[s])
        buf, so = (fin, lax.rem(u, NF)) if s == 4 else (acc, sl)
        buf[so, r] = (acc[sl, r].astype(jnp.float32) + rbs[s][k, lax.rem(u, K)].astype(jnp.float32)).astype(jnp.bfloat16)

    def tick(t, _):
        def ev(e, f):
            u = t - o[e]
            @pl.when(jnp.logical_and(u >= 0, u < nu))
            def _():
                f(u)
        def e10(u):
            cp_d(u).wait(); cp_st(u).wait()
        def e9(u):
            for k in range(2): cp_ag(u, k, 1).wait()
            cp_d(u).start(); cp_st(u).start()
        def mk_ag(s):
            def f(u):
                for k in range(2): cp_ag(u, k, s).wait()
                for k in range(2): cp_ag(u, k, s - 1).start()
            return f
        def e5(u):
            for k in range(2):
                cp_rs(u, k, 4).wait(); add_rs(u, k, 4)
            for k in range(2): cp_ag(u, k, 4).start()
        def mk_rs(s):
            def f(u):
                for k in range(2):
                    cp_rs(u, k, s - 1).wait(); add_rs(u, k, s - 1)
                for k in range(2): cp_rs(u, k, s).start()
            return f
        def e1(u):
            cp_c(u).wait(); add_c(u)
            for k in range(2): cp_rs(u, k, 1).start()
        def e0(u):
            cp_c(u).start()
        ev(10, e10); ev(9, e9)
        for e, s in ((8, 2), (7, 3), (6, 4)): ev(e, mk_ag(s))
        ev(5, e5)
        for e in (4, 3, 2): ev(e, mk_rs(e))
        ev(1, e1); ev(0, e0)
        return 0
    def cp_w(step, k):
        sl = lax.rem(step, 2)
        src, dst = ((w_up, wup), (w_dn, wdn))[k]
        return pltpu.make_async_copy(src.at[layers - 1 - step], dst.at[sl], w_s.at[k, sl])
    n = w_up.shape[2] // 4
    d2 = h_last.shape[1] // 2
    def chunk(step, q):
        sl = lax.rem(step, 2)
        @pl.when(jnp.logical_and(q == 0, step <= layers))
        def _():
            c_low[...] = c_state[...].astype(bf)
        @pl.when(jnp.logical_and(q == 0, step < layers))
        def _():
            for k in range(2): cp_w(step, k).wait()
        @pl.when(jnp.logical_and(q == 0, step < layers - 1))
        def _():
            for k in range(2): cp_w(step + 1, k).start()
        @pl.when(step < layers)
        def _():
            cols = pl.ds(pl.multiple_of(q * n, n), n)
            pin = p_all[layers - 1 - step]
            wu = wup[sl, :, cols].astype(bf)
            act, back = jax.vjp(gelu_tanh, dot(pin, wu))
            ac = lax.dot_general(c_low[...], wdn[sl, cols, :].astype(bf), NT, preferred_element_type=f32)
            pre = back(ac)[0].astype(bf)
            gd = lax.dot_general(act.astype(bf), c_low[...], TN, preferred_element_type=f32).astype(bf)
            gu = lax.dot_general(pin, pre, TN, preferred_element_type=f32).astype(bf)
            for t in range(2):
                g[sl, q, t] = gu[:, t * d2:(t + 1) * d2]
                g[sl, 4 + 2 * (q // 2) + t, lax.rem(q, 2)] = gd[:, t * d2:(t + 1) * d2]
            c_state[...] += lax.dot_general(pre, wu, NT, preferred_element_type=f32)
        @pl.when(step == layers)
        def _():
            for r in range(2):
                xs = x[:, pl.ds(pl.multiple_of((2 * q + r) * tr, tr), tr)]
                gi = lax.dot_general(xs, c_low[...], TN, preferred_element_type=f32).astype(bf)
                for t in range(2):
                    g[sl, 2 * q + t, r] = gi[:, t * d2:(t + 1) * d2]
    for k in range(2): cp_w(0, k).start()
    c_state[...] = (h_last[...] - y[...].astype(f32)) / scale
    def block(b, _):
        lax.fori_loop(2 * b - 8, 2 * b - 6, tick, 0)
        chunk(b // 4, lax.rem(b, 4))
        return 0
    lax.fori_loop(0, 4 + (nu + o[10] + 1) // 2, block, 0)

def backward_sum(scale, x, y, h_last, p_all, w_up, w_down, lags=(1, (3, 3, 3, 3), (3, 3, 3, 3), 1), orders=("xayb", "yaxb"), cid=0):
    layers, d, ff = w_up.shape
    nu, tr, tw = 8 * (layers + 1), 512, d // 2
    l0, lrs, lag_, ld = lags
    K = 2 * max(l0, ld, *lrs, *lag_)
    NS = l0 + sum(lrs)
    NF = sum(lrs) + sum(lag_) + ld
    half = tr // 2
    vm = pl.BlockSpec(memory_space=pltpu.VMEM)
    hb = pl.BlockSpec(memory_space=pl.ANY)
    return pl.pallas_call(
        functools.partial(back_sum_kernel, layers, scale, nu, tr, tw, lags, orders),
        out_shape=jax.ShapeDtypeStruct((nu, 2, tr, tw), bf),
        in_specs=[vm, vm, vm, vm, hb, hb],
        out_specs=hb,
        scratch_shapes=[pltpu.VMEM(h_last.shape, f32), pltpu.VMEM(h_last.shape, bf), pltpu.VMEM((2, d, ff), f32), pltpu.VMEM((2, ff, d), f32),
                        pltpu.SemaphoreType.DMA((2, 2)), pltpu.VMEM((2, 8, 2, tr, tw), bf),
                        pltpu.VMEM((NS, tr, tw), bf), pltpu.VMEM((NF, tr, tw), bf), pltpu.VMEM((K, tr, tw), bf)]
        + [pltpu.VMEM((2, K, half >> s, tw), bf) for s in range(1, 5)]
        + [pltpu.SemaphoreType.DMA((K,))] * 2 + [pltpu.SemaphoreType.DMA((4, 2, K))] * 4 + [pltpu.SemaphoreType.DMA((K,))] * 3,
        compiler_params=pltpu.CompilerParams(collective_id=cid, has_side_effects=True, vmem_limit_bytes=62 * 2**20),
        name="backward_sum",
    )(x, y, h_last, p_all, w_up, w_down)

def fwd_kernel(layers, x, w_in, w_up, w_down, p_out, h_out, h):
    i = pl.program_id(0)
    @pl.when(i < 4)
    def _():
        kq = x.shape[1]
        part = dot(x[...], w_in[...].astype(bf))
        @pl.when(i == 0)
        def _(): h[...] = part
        @pl.when(i > 0)
        def _(): h[...] += part
    @pl.when(i >= 4)
    def _():
        p = h[...].astype(bf)
        p_out[0] = p
        n = w_up.shape[2] // 4
        for q in range(4):
            c = slice(q * n, (q + 1) * n)
            u = dot(p, w_up[0, :, c].astype(bf))
            a = gelu_tanh(u).astype(bf)
            h[...] += dot(a, w_down[0, c, :].astype(bf))
    @pl.when(i == layers + 3)
    def _(): h_out[...] = h[...]

def forward(x, w_in, w_up, w_down):
    rows, e = x.shape
    layers, d, ff = w_up.shape
    lay = lambda i: jnp.maximum(i - 4, 0)
    return pl.pallas_call(
        functools.partial(fwd_kernel, layers), grid=(layers + 4,),
        out_shape=[jax.ShapeDtypeStruct((layers, rows, d), bf), jax.ShapeDtypeStruct((rows, d), f32)],
        in_specs=[pl.BlockSpec((rows, e // 4), lambda i: (0, jnp.minimum(i, 3))), pl.BlockSpec((e // 4, d), lambda i: (jnp.minimum(i, 3), 0)),
                  pl.BlockSpec((1, d, ff), lambda i: (lay(i), 0, 0)), pl.BlockSpec((1, ff, d), lambda i: (lay(i), 0, 0))],
        out_specs=[pl.BlockSpec((1, rows, d), lambda i: (lay(i), 0, 0)), pl.BlockSpec((rows, d), lambda i: (0, 0))],
        scratch_shapes=[pltpu.VMEM((rows, d), f32)],
        compiler_params=pltpu.CompilerParams(vmem_limit_bytes=60 * 2**20), name="forward",
    )(x, w_in, w_up, w_down)

def upd_kernel(layers, eta, mu, x, y, g, w_in, w_up, w_down, m_in, m_up, m_down,
               nw_in, nw_up, nw_down, nm_in, nm_up, nm_down, loss, h_out, h, p, a):
    i = pl.program_id(0)
    d = h.shape[1]
    d2 = d // 2
    v = i - 4
    r = lax.rem(jnp.maximum(v, 0), 4)
    def upd(w, m, nw, nm, u, t, ix):
        nmv = mu * m[ix] + g[u, t].astype(f32)
        nm[ix] = nmv
        nwv = w[ix] - eta * nmv
        nw[ix] = nwv
        return nwv.astype(bf)
    @pl.when(i < 4)
    def _():
        for j in range(2):
            cols = slice(j * d2, (j + 1) * d2)
            tot = None
            for t in range(2):
                s = slice(512 * t, 512 * (t + 1))
                q = dot(x[:, s], upd(w_in, m_in, nw_in, nm_in, j, t, (s, cols)))
                tot = q if tot is None else tot + q
            @pl.when(i == 0)
            def _(): h[:, cols] = tot
            @pl.when(i > 0)
            def _(): h[:, cols] += tot
    @pl.when(jnp.logical_and(v >= 0, r == 0))
    def _(): p[...] = h[...].astype(bf)
    @pl.when(jnp.logical_and(v >= 0, r < 2))
    def _():
        for j in range(2):
            for t in range(2):
                s = slice(512 * j + d2 * t, 512 * j + d2 * (t + 1))
                wl = upd(w_up, m_up, nw_up, nm_up, j, t, (0, slice(None), s))
                a[r, :, s] = gelu_tanh(dot(p[...], wl)).astype(bf)
    @pl.when(jnp.logical_and(v >= 0, r >= 2))
    def _():
        for j in range(2):
            cols = slice(j * d2, (j + 1) * d2)
            tot = None
            for t in range(2):
                s = slice(512 * t, 512 * (t + 1))
                q = dot(a[r - 2, :, s], upd(w_down, m_down, nw_down, nm_down, j, t, (0, s, cols)))
                tot = q if tot is None else tot + q
            h[:, cols] += tot
    @pl.when(i == 4 * layers + 3)
    def _():
        h_out[...] = h[...]
        e = h[...] - y[...].astype(f32)
        loss[...] = jnp.sum(e * e, axis=1, keepdims=True) / (2 * d)

def update(eta, mu, x, y, g, w_in, w_up, w_down, m_in, m_up, m_down):
    rows, e = x.shape
    layers, d, ff = w_up.shape
    nu = 8 * (layers + 1)
    q4 = lambda i: jnp.maximum(i - 4, 0)
    s_in = pl.BlockSpec((1024, d), lambda i: (jnp.minimum(i, 3), 0))
    s_up = pl.BlockSpec((1, d, 1024), lambda i: (q4(i) // 4, 0, jnp.minimum(lax.rem(q4(i), 4), 1)))
    s_dn = pl.BlockSpec((1, 1024, d), lambda i: (q4(i) // 4, jnp.maximum(lax.rem(q4(i), 4) - 2, 0), 0))
    x_spec = pl.BlockSpec((rows, 1024), lambda i: (0, jnp.minimum(i, 3)))
    full = pl.BlockSpec((rows, d), lambda i: (0, 0))
    o = [jax.ShapeDtypeStruct(t.shape, f32) for t in (w_in, w_up, w_down, m_in, m_up, m_down)]
    o += [jax.ShapeDtypeStruct((rows, 1), f32), jax.ShapeDtypeStruct((rows, d), f32)]
    return pl.pallas_call(
        functools.partial(upd_kernel, layers, eta, mu), grid=(nu // 2,), out_shape=o,
        in_specs=[x_spec, full, pl.BlockSpec((2, 2, 512, d // 2), lambda i: (i, 0, 0, 0)), s_in, s_up, s_dn, s_in, s_up, s_dn],
        out_specs=[s_in, s_up, s_dn, s_in, s_up, s_dn, pl.BlockSpec((rows, 1), lambda i: (0, 0)), full],
        scratch_shapes=[pltpu.VMEM((rows, d), f32), pltpu.VMEM((rows, d), bf), pltpu.VMEM((2, rows, 1024), bf)],
        compiler_params=pltpu.CompilerParams(vmem_limit_bytes=63 * 2**20), name="update",
    )(x, y, g, w_in, w_up, w_down, m_in, m_up, m_down)


def solution(mesh):
    group_size = mesh.shape["data"]

    def device_steps(w_in, w_up, w_down, mom_in, mom_up, mom_down, x_now, y_now, x_next, y_next):
        local_rows, model_width = y_now.shape
        step_size = 4.0 * model_width / (w_up.shape[2] * (w_up.shape[0] + 1))
        p_all, h_last = forward(x_now, w_in, w_up, w_down)
        total = backward_sum(float(local_rows * group_size * model_width), x_now, y_now, h_last, p_all, w_up, w_down)
        out = update(step_size, MOMENTUM, x_next, y_next, total, w_in, w_up, w_down, mom_in, mom_up, mom_down)
        return (*out[:6], out[6][:, 0], out[7])

    row_spec = P("data", None)
    return jax.shard_map(
        device_steps,
        mesh=mesh,
        in_specs=(P(),) * 6 + (row_spec,) * 4,
        out_specs=(P(),) * 6 + (P("data"), row_spec),
        check_vma=False,
    )
```

```python
import functools

import jax
import jax.numpy as jnp
from jax import lax
from jax.experimental import pallas as pl
from jax.experimental.pallas import tpu as pltpu
from jax.sharding import PartitionSpec as P

MOMENTUM = 0.9
MESH = pl.DeviceIdType.MESH
BIT = {"c": 1, "x": 2, "y": 4, "a": 8, "b": 16}

bf, f32 = jnp.bfloat16, jnp.float32
TN = (((0,), (0,)), ((), ()))
NT = (((1,), (1,)), ((), ()))
def dot(a, b): return jnp.dot(a, b, preferred_element_type=f32)
def gelu_tanh(v): return jax.nn.gelu(v, approximate=True)

def back_sum_kernel(layers, scale, nu, tr, tw, lags, *refs):
    (x, y, h_last, p_all, w_up, w_dn, gs, c_state, c_low, wup, wdn, w_s, g, acc, fin, rb0, rb1, rb3, rzu, rzd,
     c_s, c_r, b_s, b_r, s_s, s_r, zr_s, zr_r, za_s, za_r, t_s, t_r, v_s, v_r, d_s, d_r, st_s) = refs
    K, KZ, NS, NF = c_s.shape[0], rzu.shape[1], acc.shape[0], fin.shape[0]
    l0, lx, lz, ly, ld = lags
    me = lax.axis_index("data")
    bit = {"c": lax.rem(me, 2), "x": lax.rem(me // 2, 2), "y": lax.rem(me // 4, 2)}
    peer = {d: me + w * (1 - 2 * bit[d]) for d, w in (("c", 1), ("x", 2), ("y", 4))}
    z = me // 8
    bar = pltpu.get_barrier_semaphore()
    def greet(dev):
        pl.semaphore_signal(bar, inc=1, device_id=(dev,), device_id_type=MESH)
    for d in "cxy":
        greet(peer[d])
    pl.when(z < 3)(lambda: greet(me + 8))
    pl.when(z > 0)(lambda: greet(me - 8))
    pl.semaphore_wait(bar, 3 + jnp.minimum(z, 1) + jnp.minimum(3 - z, 1))
    half, big, ch = tr // 2, tr // 4, tr // 16
    small = ch // 2
    D1, D2 = "xy", "yx"
    base0 = [0, half]
    base1 = [base0[k] + big * bit[D1[k]] for k in range(2)]
    give1 = [base0[k] + big * (1 - bit[D1[k]]) for k in range(2)]
    base3 = [base1[k] + ch * z + small * bit[D2[k]] for k in range(2)]
    give3 = [base1[k] + ch * z + small * (1 - bit[D2[k]]) for k in range(2)]
    o1 = l0
    o2 = o1 + lx
    o3 = o2 + 3 * lz
    o4 = o3 + ly
    o5 = o4 + ly
    o6 = o5 + 3 * lz
    o7 = o6 + lx
    o8 = o7 + ld
    assert NS >= o4 and NF >= o8 - o1
    def rows(off, n):
        return pl.ds(pl.multiple_of(off, min(16, small)), n)
    def remote(src, dst, ss, rs, dev):
        return pltpu.make_async_remote_copy(src_ref=src, dst_ref=dst, send_sem=ss, recv_sem=rs, device_id=(dev,), device_id_type=MESH)
    def ix(u): return lax.rem(u, K)
    def iz(u): return lax.rem(u, KZ)
    def accr(u, off, n): return acc.at[lax.rem(u, NS), rows(off, n)]
    def finr(u, off, n): return fin.at[lax.rem(u, NF), rows(off, n)]
    def own(u): return lax.rem(u // 8, 2), lax.rem(u, 8)
    def out(u): return nu - 8 - 8 * (u // 8) + lax.rem(u, 8)
    def cp_c(u):
        return remote(g.at[(*own(u), 1 - bit["c"])], rb0.at[ix(u)], c_s.at[ix(u)], c_r.at[ix(u)], peer["c"])
    def cp_b(u, k):
        return remote(accr(u, give1[k], big), rb1.at[k, ix(u)], b_s.at[k, ix(u)], b_r.at[k, ix(u)], peer[D1[k]])
    def cp_s(u, k):
        return remote(accr(u, give3[k], small), rb3.at[k, ix(u)], s_s.at[k, ix(u)], s_r.at[k, ix(u)], peer[D2[k]])
    def cp_v(u, k):
        r = finr(u, base3[k], small)
        return remote(r, r, v_s.at[k, ix(u)], v_r.at[k, ix(u)], peer[D2[k]])
    def cp_t(u, k):
        r = finr(u, base1[k], big)
        return remote(r, r, t_s.at[k, ix(u)], t_r.at[k, ix(u)], peer[D1[k]])
    def cp_d(u):
        return remote(fin.at[lax.rem(u, NF)], gs.at[out(u), bit["c"]], d_s.at[ix(u)], d_r.at[ix(u)], peer["c"])
    def cp_st(u):
        return pltpu.make_async_copy(fin.at[lax.rem(u, NF)], gs.at[out(u), bit["c"]], st_s.at[ix(u)])
    def cp_zr(u, k, side, f, n):
        buf = (rzu, rzd)[side].at[k, iz(u), pl.ds(0, n * ch)]
        return remote(accr(u, base1[k] + ch * f, n * ch), buf, zr_s.at[side, k, iz(u)], zr_r.at[side, k, iz(u)], me + (8, -8)[side])
    def cp_za(u, k, side, f, n):
        r = finr(u, base1[k] + ch * f, n * ch)
        return remote(r, r, za_s.at[side, k, iz(u)], za_r.at[side, k, iz(u)], me + (8, -8)[side])
    snd_r = [lambda q: (q + 1, 3 - q), lambda q: (0, q)]
    rcv_r = [lambda q: (q, 4 - q), lambda q: (0, q + 1)]
    snd_a = [lambda q: (0, q + 1), lambda q: (q, 4 - q)]
    rcv_a = [lambda q: (0, q), lambda q: (q + 1, 3 - q)]
    senders, takers = [(0, 1, 2), (1, 2, 3)], [(1, 2, 3), (0, 1, 2)]
    def add(dst, slot, r, a, b):
        dst[slot, r] = (a.astype(f32) + b.astype(f32)).astype(bf)
    def tick(t, _):
        def ev(off, f):
            u = t - off
            pl.when(jnp.logical_and(u >= 0, u < nu))(lambda: f(u))
        def pair(cp, what):
            def f(u):
                for k in range(2): getattr(cp(u, k), what)()
            return f
        def line(o, cp, snd, rcv, take):
            at = [o + z * lz, o + (3 - z) * lz]
            for side in range(2):
                for q in senders[side]:
                    def sent(u, side=side, q=q):
                        for k in range(2): cp(u, k, side, *snd[side](q)).wait_send()
                    pl.when(z == q)(lambda: ev(at[side] + lz, sent))
                for q in takers[side]:
                    def got(u, side=side, q=q):
                        for k in range(2):
                            cp(u, k, side, *rcv[side](q)).wait_recv()
                            take(u, k, side, *rcv[side](q))
                    pl.when(z == q)(lambda: ev(at[side], got))
            for side in range(2):
                for q in senders[side]:
                    def send(u, side=side, q=q):
                        for k in range(2): cp(u, k, side, *snd[side](q)).start()
                    pl.when(z == q)(lambda: ev(at[side], send))
        def take_r(u, k, side, f, n):
            r = rows(base1[k] + ch * f, n * ch)
            add(acc, lax.rem(u, NS), r, acc[lax.rem(u, NS), r], (rzu, rzd)[side][k, iz(u), 0:n * ch])
        def take_a(u, k, side, f, n):
            pass
        def e8(u):
            cp_d(u).wait(); cp_st(u).wait()
        def e7(u):
            pair(cp_t, "wait")(u)
            cp_d(u).start(); cp_st(u).start()
        def e4(u):
            for k in range(2):
                cp_s(u, k).wait()
                r = rows(base3[k], small)
                add(fin, lax.rem(u, NF), r, acc[lax.rem(u, NS), r], rb3[k, ix(u)])
            pair(cp_v, "start")(u)
        def e2(u):
            for k in range(2):
                cp_b(u, k).wait()
                r = rows(base1[k], big)
                add(acc, lax.rem(u, NS), r, acc[lax.rem(u, NS), r], rb1[k, ix(u)])
        def e1(u):
            cp_c(u).wait()
            so, uo = own(u)
            for h in range(4):
                r = slice(h * big, (h + 1) * big)
                add(acc, lax.rem(u, NS), r, g[so, uo, bit["c"], r], rb0[ix(u), r])
            pair(cp_b, "start")(u)
        ev(o8, e8)
        ev(o7, e7)
        ev(o5, pair(cp_v, "wait"))
        line(o5, cp_za, snd_a, rcv_a, take_a)
        ev(o6, pair(cp_t, "start"))
        ev(o4, e4)
        ev(o2, e2)
        line(o2, cp_zr, snd_r, rcv_r, take_r)
        ev(o3, pair(cp_s, "start"))
        ev(o1, e1)
        ev(0, lambda u: cp_c(u).start())
        return 0
    def cp_w(step, k):
        sl = lax.rem(step, 2)
        src, dst = ((w_up, wup), (w_dn, wdn))[k]
        return pltpu.make_async_copy(src.at[layers - 1 - step], dst.at[sl], w_s.at[k, sl])
    n = w_up.shape[2] // 4
    d2 = h_last.shape[1] // 2
    def chunk(step, q):
        sl = lax.rem(step, 2)
        @pl.when(jnp.logical_and(q == 0, step <= layers))
        def _():
            c_low[...] = c_state[...].astype(bf)
        @pl.when(jnp.logical_and(q == 0, step < layers))
        def _():
            for k in range(2): cp_w(step, k).wait()
        @pl.when(jnp.logical_and(q == 0, step < layers - 1))
        def _():
            for k in range(2): cp_w(step + 1, k).start()
        @pl.when(step < layers)
        def _():
            cols = pl.ds(pl.multiple_of(q * n, n), n)
            pin = p_all[layers - 1 - step]
            wu = wup[sl, :, cols].astype(bf)
            act, back = jax.vjp(gelu_tanh, dot(pin, wu))
            ac = lax.dot_general(c_low[...], wdn[sl, cols, :].astype(bf), NT, preferred_element_type=f32)
            pre = back(ac)[0].astype(bf)
            gd = lax.dot_general(act.astype(bf), c_low[...], TN, preferred_element_type=f32).astype(bf)
            gu = lax.dot_general(pin, pre, TN, preferred_element_type=f32).astype(bf)
            for t in range(2):
                g[sl, q, t] = gu[:, t * d2:(t + 1) * d2]
                g[sl, 4 + 2 * (q // 2) + t, lax.rem(q, 2)] = gd[:, t * d2:(t + 1) * d2]
            c_state[...] += lax.dot_general(pre, wu, NT, preferred_element_type=f32)
        @pl.when(step == layers)
        def _():
            for r in range(2):
                xs = x[:, pl.ds(pl.multiple_of((2 * q + r) * tr, tr), tr)]
                gi = lax.dot_general(xs, c_low[...], TN, preferred_element_type=f32).astype(bf)
                for t in range(2):
                    g[sl, 2 * q + t, r] = gi[:, t * d2:(t + 1) * d2]
    for k in range(2): cp_w(0, k).start()
    c_state[...] = (h_last[...] - y[...].astype(f32)) / scale
    def block(b, _):
        lax.fori_loop(2 * b - 8, 2 * b - 6, tick, 0)
        chunk(b // 4, lax.rem(b, 4))
        return 0
    lax.fori_loop(0, 4 + (nu + o8 + 1) // 2, block, 0)

def backward_sum(scale, x, y, h_last, p_all, w_up, w_down, lags=(1, 2, 2, 2, 1), cid=0):
    layers, d, ff = w_up.shape
    nu, tr, tw = 8 * (layers + 1), 512, d // 2
    l0, lx, lz, ly, ld = lags
    K = 2 * max(lags)
    KZ = 3 * max(lags)
    NS = l0 + lx + 3 * lz + ly
    NF = 2 * lx + 6 * lz + 2 * ly + ld
    vm = pl.BlockSpec(memory_space=pltpu.VMEM)
    hb = pl.BlockSpec(memory_space=pl.ANY)
    sem = pltpu.SemaphoreType.DMA
    return pl.pallas_call(
        functools.partial(back_sum_kernel, layers, scale, nu, tr, tw, lags),
        out_shape=jax.ShapeDtypeStruct((nu, 2, tr, tw), bf),
        in_specs=[vm, vm, vm, vm, hb, hb],
        out_specs=hb,
        scratch_shapes=[pltpu.VMEM(h_last.shape, f32), pltpu.VMEM(h_last.shape, bf), pltpu.VMEM((2, d, ff), f32), pltpu.VMEM((2, ff, d), f32),
                        sem((2, 2)), pltpu.VMEM((2, 8, 2, tr, tw), bf),
                        pltpu.VMEM((NS, tr, tw), bf), pltpu.VMEM((NF, tr, tw), bf), pltpu.VMEM((K, tr, tw), bf),
                        pltpu.VMEM((2, K, tr // 4, tw), bf), pltpu.VMEM((2, K, tr // 32, tw), bf),
                        pltpu.VMEM((2, KZ, 3 * tr // 16, tw), bf), pltpu.VMEM((2, KZ, 3 * tr // 16, tw), bf)]
        + [sem((K,))] * 2 + [sem((2, K))] * 4 + [sem((2, 2, KZ))] * 4 + [sem((2, K))] * 4 + [sem((K,))] * 3,
        compiler_params=pltpu.CompilerParams(collective_id=cid, has_side_effects=True, vmem_limit_bytes=62 * 2**20),
        name="backward_sum",
    )(x, y, h_last, p_all, w_up, w_down)

def fwd_kernel(layers, x, w_in, w_up, w_down, p_out, h_out, h):
    i = pl.program_id(0)
    @pl.when(i < 4)
    def _():
        kq = x.shape[1]
        part = dot(x[...], w_in[...].astype(bf))
        @pl.when(i == 0)
        def _(): h[...] = part
        @pl.when(i > 0)
        def _(): h[...] += part
    @pl.when(i >= 4)
    def _():
        p = h[...].astype(bf)
        p_out[0] = p
        n = w_up.shape[2] // 4
        for q in range(4):
            c = slice(q * n, (q + 1) * n)
            u = dot(p, w_up[0, :, c].astype(bf))
            a = gelu_tanh(u).astype(bf)
            h[...] += dot(a, w_down[0, c, :].astype(bf))
    @pl.when(i == layers + 3)
    def _(): h_out[...] = h[...]

def forward(x, w_in, w_up, w_down):
    rows, e = x.shape
    layers, d, ff = w_up.shape
    lay = lambda i: jnp.maximum(i - 4, 0)
    return pl.pallas_call(
        functools.partial(fwd_kernel, layers), grid=(layers + 4,),
        out_shape=[jax.ShapeDtypeStruct((layers, rows, d), bf), jax.ShapeDtypeStruct((rows, d), f32)],
        in_specs=[pl.BlockSpec((rows, e // 4), lambda i: (0, jnp.minimum(i, 3))), pl.BlockSpec((e // 4, d), lambda i: (jnp.minimum(i, 3), 0)),
                  pl.BlockSpec((1, d, ff), lambda i: (lay(i), 0, 0)), pl.BlockSpec((1, ff, d), lambda i: (lay(i), 0, 0))],
        out_specs=[pl.BlockSpec((1, rows, d), lambda i: (lay(i), 0, 0)), pl.BlockSpec((rows, d), lambda i: (0, 0))],
        scratch_shapes=[pltpu.VMEM((rows, d), f32)],
        compiler_params=pltpu.CompilerParams(vmem_limit_bytes=60 * 2**20), name="forward",
    )(x, w_in, w_up, w_down)

def upd_kernel(layers, eta, mu, x, y, g, w_in, w_up, w_down, m_in, m_up, m_down,
               nw_in, nw_up, nw_down, nm_in, nm_up, nm_down, loss, h_out, h, p, a):
    i = pl.program_id(0)
    d = h.shape[1]
    d2 = d // 2
    v = i - 4
    r = lax.rem(jnp.maximum(v, 0), 4)
    def upd(w, m, nw, nm, u, t, ix):
        nmv = mu * m[ix] + g[u, t].astype(f32)
        nm[ix] = nmv
        nwv = w[ix] - eta * nmv
        nw[ix] = nwv
        return nwv.astype(bf)
    @pl.when(i < 4)
    def _():
        for j in range(2):
            cols = slice(j * d2, (j + 1) * d2)
            tot = None
            for t in range(2):
                s = slice(512 * t, 512 * (t + 1))
                q = dot(x[:, s], upd(w_in, m_in, nw_in, nm_in, j, t, (s, cols)))
                tot = q if tot is None else tot + q
            @pl.when(i == 0)
            def _(): h[:, cols] = tot
            @pl.when(i > 0)
            def _(): h[:, cols] += tot
    @pl.when(jnp.logical_and(v >= 0, r == 0))
    def _(): p[...] = h[...].astype(bf)
    @pl.when(jnp.logical_and(v >= 0, r < 2))
    def _():
        for j in range(2):
            for t in range(2):
                s = slice(512 * j + d2 * t, 512 * j + d2 * (t + 1))
                wl = upd(w_up, m_up, nw_up, nm_up, j, t, (0, slice(None), s))
                a[r, :, s] = gelu_tanh(dot(p[...], wl)).astype(bf)
    @pl.when(jnp.logical_and(v >= 0, r >= 2))
    def _():
        for j in range(2):
            cols = slice(j * d2, (j + 1) * d2)
            tot = None
            for t in range(2):
                s = slice(512 * t, 512 * (t + 1))
                q = dot(a[r - 2, :, s], upd(w_down, m_down, nw_down, nm_down, j, t, (0, s, cols)))
                tot = q if tot is None else tot + q
            h[:, cols] += tot
    @pl.when(i == 4 * layers + 3)
    def _():
        h_out[...] = h[...]
        e = h[...] - y[...].astype(f32)
        loss[...] = jnp.sum(e * e, axis=1, keepdims=True) / (2 * d)

def update(eta, mu, x, y, g, w_in, w_up, w_down, m_in, m_up, m_down):
    rows, e = x.shape
    layers, d, ff = w_up.shape
    nu = 8 * (layers + 1)
    q4 = lambda i: jnp.maximum(i - 4, 0)
    s_in = pl.BlockSpec((1024, d), lambda i: (jnp.minimum(i, 3), 0))
    s_up = pl.BlockSpec((1, d, 1024), lambda i: (q4(i) // 4, 0, jnp.minimum(lax.rem(q4(i), 4), 1)))
    s_dn = pl.BlockSpec((1, 1024, d), lambda i: (q4(i) // 4, jnp.maximum(lax.rem(q4(i), 4) - 2, 0), 0))
    x_spec = pl.BlockSpec((rows, 1024), lambda i: (0, jnp.minimum(i, 3)))
    full = pl.BlockSpec((rows, d), lambda i: (0, 0))
    o = [jax.ShapeDtypeStruct(t.shape, f32) for t in (w_in, w_up, w_down, m_in, m_up, m_down)]
    o += [jax.ShapeDtypeStruct((rows, 1), f32), jax.ShapeDtypeStruct((rows, d), f32)]
    return pl.pallas_call(
        functools.partial(upd_kernel, layers, eta, mu), grid=(nu // 2,), out_shape=o,
        in_specs=[x_spec, full, pl.BlockSpec((2, 2, 512, d // 2), lambda i: (i, 0, 0, 0)), s_in, s_up, s_dn, s_in, s_up, s_dn],
        out_specs=[s_in, s_up, s_dn, s_in, s_up, s_dn, pl.BlockSpec((rows, 1), lambda i: (0, 0)), full],
        scratch_shapes=[pltpu.VMEM((rows, d), f32), pltpu.VMEM((rows, d), bf), pltpu.VMEM((2, rows, 1024), bf)],
        compiler_params=pltpu.CompilerParams(vmem_limit_bytes=63 * 2**20), name="update",
    )(x, y, g, w_in, w_up, w_down, m_in, m_up, m_down)


def solution(mesh):
    group_size = mesh.shape["data"]

    def device_steps(w_in, w_up, w_down, mom_in, mom_up, mom_down, x_now, y_now, x_next, y_next):
        local_rows, model_width = y_now.shape
        step_size = 4.0 * model_width / (w_up.shape[2] * (w_up.shape[0] + 1))
        p_all, h_last = forward(x_now, w_in, w_up, w_down)
        total = backward_sum(float(local_rows * group_size * model_width), x_now, y_now, h_last, p_all, w_up, w_down)
        out = update(step_size, MOMENTUM, x_next, y_next, total, w_in, w_up, w_down, mom_in, mom_up, mom_down)
        return (*out[:6], out[6][:, 0], out[7])

    row_spec = P("data", None)
    return jax.shard_map(
        device_steps,
        mesh=mesh,
        in_specs=(P(),) * 6 + (row_spec,) * 4,
        out_specs=(P(),) * 6 + (P("data"), row_spec),
        check_vma=False,
    )
```

```python
import functools

import jax
import jax.numpy as jnp
from jax import lax
from jax.experimental import pallas as pl
from jax.experimental.pallas import tpu as pltpu
from jax.sharding import PartitionSpec as P

MOMENTUM = 0.9
MESH = pl.DeviceIdType.MESH
BIT = {"c": 1, "x": 2, "y": 4, "a": 8, "b": 16}

bf, f32 = jnp.bfloat16, jnp.float32
TN = (((0,), (0,)), ((), ()))
NT = (((1,), (1,)), ((), ()))
def dot(a, b): return jnp.dot(a, b, preferred_element_type=f32)
def gelu_tanh(v): return jax.nn.gelu(v, approximate=True)

def grad_sum_kernel(layers, scale, nu, tr, tw, lags, *refs):
    (x_hbm, y, w_in, w_up, w_dn, gs, x, p_all, c_state, c_low, wup, wdn, w_s, x_s, g, acc, fin, rb0, rb1, rb3, rzu, rzd,
     c_s, c_r, b_s, b_r, s_s, s_r, zr_s, zr_r, za_s, za_r, t_s, t_r, v_s, v_r, d_s, d_r, st_s) = refs
    K, KZ, NS, NF = c_s.shape[0], rzu.shape[1], acc.shape[0], fin.shape[0]
    l0, lx, lz, ly, ld = lags
    me = lax.axis_index("data")
    bit = {"c": lax.rem(me, 2), "x": lax.rem(me // 2, 2), "y": lax.rem(me // 4, 2)}
    peer = {d: me + w * (1 - 2 * bit[d]) for d, w in (("c", 1), ("x", 2), ("y", 4))}
    z = me // 8
    bar = pltpu.get_barrier_semaphore()
    def greet(dev):
        pl.semaphore_signal(bar, inc=1, device_id=(dev,), device_id_type=MESH)
    for d in "cxy":
        greet(peer[d])
    pl.when(z < 3)(lambda: greet(me + 8))
    pl.when(z > 0)(lambda: greet(me - 8))
    half, big, ch = tr // 2, tr // 4, tr // 16
    small = ch // 2
    D1, D2 = "xy", "yx"
    base0 = [0, half]
    base1 = [base0[k] + big * bit[D1[k]] for k in range(2)]
    give1 = [base0[k] + big * (1 - bit[D1[k]]) for k in range(2)]
    base3 = [base1[k] + ch * z + small * bit[D2[k]] for k in range(2)]
    give3 = [base1[k] + ch * z + small * (1 - bit[D2[k]]) for k in range(2)]
    o1 = l0
    o2 = o1 + lx
    o3 = o2 + 3 * lz
    o4 = o3 + ly
    o5 = o4 + ly
    o6 = o5 + 3 * lz
    o7 = o6 + lx
    o8 = o7 + ld
    assert NS >= o4 and NF >= o8 - o1
    def rows(off, n):
        return pl.ds(pl.multiple_of(off, min(16, small)), n)
    def remote(src, dst, ss, rs, dev):
        return pltpu.make_async_remote_copy(src_ref=src, dst_ref=dst, send_sem=ss, recv_sem=rs, device_id=(dev,), device_id_type=MESH)
    def ix(u): return lax.rem(u, K)
    def iz(u): return lax.rem(u, KZ)
    def accr(u, off, n): return acc.at[lax.rem(u, NS), rows(off, n)]
    def finr(u, off, n): return fin.at[lax.rem(u, NF), rows(off, n)]
    def own(u): return lax.rem(u // 8, 2), lax.rem(u, 8)
    def out(u): return nu - 8 - 8 * (u // 8) + lax.rem(u, 8)
    def cp_c(u):
        return remote(g.at[(*own(u), 1 - bit["c"])], rb0.at[ix(u)], c_s.at[ix(u)], c_r.at[ix(u)], peer["c"])
    def cp_b(u, k):
        return remote(accr(u, give1[k], big), rb1.at[k, ix(u)], b_s.at[k, ix(u)], b_r.at[k, ix(u)], peer[D1[k]])
    def cp_s(u, k):
        return remote(accr(u, give3[k], small), rb3.at[k, ix(u)], s_s.at[k, ix(u)], s_r.at[k, ix(u)], peer[D2[k]])
    def cp_v(u, k):
        r = finr(u, base3[k], small)
        return remote(r, r, v_s.at[k, ix(u)], v_r.at[k, ix(u)], peer[D2[k]])
    def cp_t(u, k):
        r = finr(u, base1[k], big)
        return remote(r, r, t_s.at[k, ix(u)], t_r.at[k, ix(u)], peer[D1[k]])
    def cp_d(u):
        return remote(fin.at[lax.rem(u, NF)], gs.at[out(u), bit["c"]], d_s.at[ix(u)], d_r.at[ix(u)], peer["c"])
    def cp_st(u):
        return pltpu.make_async_copy(fin.at[lax.rem(u, NF)], gs.at[out(u), bit["c"]], st_s.at[ix(u)])
    def cp_zr(u, k, side, f, n):
        buf = (rzu, rzd)[side].at[k, iz(u), pl.ds(0, n * ch)]
        return remote(accr(u, base1[k] + ch * f, n * ch), buf, zr_s.at[side, k, iz(u)], zr_r.at[side, k, iz(u)], me + (8, -8)[side])
    def cp_za(u, k, side, f, n):
        r = finr(u, base1[k] + ch * f, n * ch)
        return remote(r, r, za_s.at[side, k, iz(u)], za_r.at[side, k, iz(u)], me + (8, -8)[side])
    snd_r = [lambda q: (q + 1, 3 - q), lambda q: (0, q)]
    rcv_r = [lambda q: (q, 4 - q), lambda q: (0, q + 1)]
    snd_a = [lambda q: (0, q + 1), lambda q: (q, 4 - q)]
    rcv_a = [lambda q: (0, q), lambda q: (q + 1, 3 - q)]
    senders, takers = [(0, 1, 2), (1, 2, 3)], [(1, 2, 3), (0, 1, 2)]
    def add(dst, slot, r, a, b):
        dst[slot, r] = (a.astype(f32) + b.astype(f32)).astype(bf)
    def tick(t, _):
        def ev(off, f):
            u = t - off
            pl.when(jnp.logical_and(u >= 0, u < nu))(lambda: f(u))
        def pair(cp, what):
            def f(u):
                for k in range(2): getattr(cp(u, k), what)()
            return f
        def line(o, cp, snd, rcv, take):
            at = [o + z * lz, o + (3 - z) * lz]
            for side in range(2):
                for q in senders[side]:
                    def sent(u, side=side, q=q):
                        for k in range(2): cp(u, k, side, *snd[side](q)).wait_send()
                    pl.when(z == q)(lambda: ev(at[side] + lz, sent))
                for q in takers[side]:
                    def got(u, side=side, q=q):
                        for k in range(2):
                            cp(u, k, side, *rcv[side](q)).wait_recv()
                            take(u, k, side, *rcv[side](q))
                    pl.when(z == q)(lambda: ev(at[side], got))
            for side in range(2):
                for q in senders[side]:
                    def send(u, side=side, q=q):
                        for k in range(2): cp(u, k, side, *snd[side](q)).start()
                    pl.when(z == q)(lambda: ev(at[side], send))
        def take_r(u, k, side, f, n):
            r = rows(base1[k] + ch * f, n * ch)
            add(acc, lax.rem(u, NS), r, acc[lax.rem(u, NS), r], (rzu, rzd)[side][k, iz(u), 0:n * ch])
        def take_a(u, k, side, f, n):
            pass
        def e8(u):
            cp_d(u).wait(); cp_st(u).wait()
        def e7(u):
            pair(cp_t, "wait")(u)
            cp_d(u).start(); cp_st(u).start()
        def e4(u):
            for k in range(2):
                cp_s(u, k).wait()
                r = rows(base3[k], small)
                add(fin, lax.rem(u, NF), r, acc[lax.rem(u, NS), r], rb3[k, ix(u)])
            pair(cp_v, "start")(u)
        def e2(u):
            for k in range(2):
                cp_b(u, k).wait()
                r = rows(base1[k], big)
                add(acc, lax.rem(u, NS), r, acc[lax.rem(u, NS), r], rb1[k, ix(u)])
        def e1(u):
            cp_c(u).wait()
            so, uo = own(u)
            for h in range(4):
                r = slice(h * big, (h + 1) * big)
                add(acc, lax.rem(u, NS), r, g[so, uo, bit["c"], r], rb0[ix(u), r])
            pair(cp_b, "start")(u)
        ev(o8, e8)
        ev(o7, e7)
        ev(o5, pair(cp_v, "wait"))
        line(o5, cp_za, snd_a, rcv_a, take_a)
        ev(o6, pair(cp_t, "start"))
        ev(o4, e4)
        ev(o2, e2)
        line(o2, cp_zr, snd_r, rcv_r, take_r)
        ev(o3, pair(cp_s, "start"))
        ev(o1, e1)
        ev(0, lambda u: cp_c(u).start())
        return 0
    d, ff = w_up.shape[1:]
    def cp_w(layer, k):
        sl = lax.rem(layer, 2)
        src, dst = ((w_up, wup), (w_dn, wdn))[k]
        return pltpu.make_async_copy(src.at[layer], dst.at[sl], w_s.at[k, sl])
    e4 = w_in.shape[0] // 4
    cp_x = pltpu.make_async_copy(x_hbm, x, x_s.at[4])
    cp_in = [pltpu.make_async_copy(w_in.at[pl.ds(i * e4, e4)], wdn.at[i // 2, pl.ds((i % 2) * e4, e4)], x_s.at[i]) for i in range(4)]
    cp_x.start()
    for c in cp_in: c.start()
    for l in range(2): cp_w(l, 0).start()
    cp_x.wait()
    h = c_state
    for i in range(4):
        cp_in[i].wait()
        part = dot(x[:, i * e4:(i + 1) * e4], wdn[i // 2, (i % 2) * e4:(i % 2 + 1) * e4].astype(bf))
        h[...] = part if i == 0 else h[...] + part
        if i % 2 == 1: cp_w(i // 2, 1).start()
    n = ff // 4
    def layer_fwd(l, _):
        sl = lax.rem(l, 2)
        pin = h[...].astype(bf)
        p_all[l] = pin
        tot = h[...]
        cp_w(l, 0).wait()
        acts = [gelu_tanh(dot(pin, wup[sl, :, q * n:(q + 1) * n].astype(bf))).astype(bf) for q in range(4)]
        cp_w(l, 1).wait()
        for q in range(4):
            tot = tot + dot(acts[q], wdn[sl, q * n:(q + 1) * n].astype(bf))
        h[...] = tot
        @pl.when(l < layers - 2)
        def _():
            for k in range(2): cp_w(l + 2, k).start()
        return 0
    lax.fori_loop(0, layers, layer_fwd, 0)
    c_state[...] = (h[...] - y[...].astype(f32)) / scale
    pl.semaphore_wait(bar, 3 + jnp.minimum(z, 1) + jnp.minimum(3 - z, 1))
    d2 = d // 2
    def chunk(step, q):
        gl = lax.rem(step, 2)
        layer = layers - 1 - step
        sl = lax.rem(layer, 2)
        @pl.when(jnp.logical_and(q == 0, step <= layers))
        def _():
            c_low[...] = c_state[...].astype(bf)
        @pl.when(jnp.logical_and(q == 0, jnp.logical_and(step >= 2, step < layers)))
        def _():
            for k in range(2): cp_w(layer, k).wait()
        @pl.when(jnp.logical_and(q == 0, jnp.logical_and(step >= 1, step < layers - 1)))
        def _():
            for k in range(2): cp_w(layer - 1, k).start()
        @pl.when(step < layers)
        def _():
            cols = pl.ds(pl.multiple_of(q * n, n), n)
            pin = p_all[layer]
            wu = wup[sl, :, cols].astype(bf)
            act, back = jax.vjp(gelu_tanh, dot(pin, wu))
            ac = lax.dot_general(c_low[...], wdn[sl, cols, :].astype(bf), NT, preferred_element_type=f32)
            pre = back(ac)[0].astype(bf)
            gd = lax.dot_general(act.astype(bf), c_low[...], TN, preferred_element_type=f32).astype(bf)
            gu = lax.dot_general(pin, pre, TN, preferred_element_type=f32).astype(bf)
            for t in range(2):
                g[gl, 4 * (q // 2) + lax.rem(q, 2), t] = gu[:, t * d2:(t + 1) * d2]
                g[gl, 4 * (q // 2) + 2 + t, lax.rem(q, 2)] = gd[:, t * d2:(t + 1) * d2]
            c_state[...] += lax.dot_general(pre, wu, NT, preferred_element_type=f32)
        @pl.when(step == layers)
        def _():
            for r in range(2):
                xs = x[:, pl.ds(pl.multiple_of((2 * q + r) * tr, tr), tr)]
                gi = lax.dot_general(xs, c_low[...], TN, preferred_element_type=f32).astype(bf)
                for t in range(2):
                    g[gl, 2 * q + t, r] = gi[:, t * d2:(t + 1) * d2]
    def block(b, _):
        lax.fori_loop(2 * b - 4, 2 * b - 2, tick, 0)
        chunk(b // 4, lax.rem(b, 4))
        return 0
    lax.fori_loop(0, 2 + (nu + o8 + 1) // 2, block, 0)

def gradient_sum(scale, x, y, w_in, w_up, w_down, lags=(1, 2, 2, 2, 1), cid=0):
    layers, d, ff = w_up.shape
    rows = x.shape[0]
    nu, tr, tw = 8 * (layers + 1), 512, d // 2
    l0, lx, lz, ly, ld = lags
    K = 2 * max(lags)
    KZ = 3 * max(lags)
    NS = l0 + lx + 3 * lz + ly
    NF = 2 * lx + 6 * lz + 2 * ly + ld
    vm = pl.BlockSpec(memory_space=pltpu.VMEM)
    hb = pl.BlockSpec(memory_space=pl.ANY)
    sem = pltpu.SemaphoreType.DMA
    return pl.pallas_call(
        functools.partial(grad_sum_kernel, layers, scale, nu, tr, tw, lags),
        out_shape=jax.ShapeDtypeStruct((nu, 2, tr, tw), bf),
        in_specs=[hb, vm, hb, hb, hb],
        out_specs=hb,
        scratch_shapes=[pltpu.VMEM(x.shape, bf), pltpu.VMEM((layers, rows, d), bf), pltpu.VMEM((rows, d), f32), pltpu.VMEM((rows, d), bf),
                        pltpu.VMEM((2, d, ff), f32), pltpu.VMEM((2, ff, d), f32), sem((2, 2)), sem((5,)), pltpu.VMEM((2, 8, 2, tr, tw), bf),
                        pltpu.VMEM((NS, tr, tw), bf), pltpu.VMEM((NF, tr, tw), bf), pltpu.VMEM((K, tr, tw), bf),
                        pltpu.VMEM((2, K, tr // 4, tw), bf), pltpu.VMEM((2, K, tr // 32, tw), bf),
                        pltpu.VMEM((2, KZ, 3 * tr // 16, tw), bf), pltpu.VMEM((2, KZ, 3 * tr // 16, tw), bf)]
        + [sem((K,))] * 2 + [sem((2, K))] * 4 + [sem((2, 2, KZ))] * 4 + [sem((2, K))] * 4 + [sem((K,))] * 3,
        compiler_params=pltpu.CompilerParams(collective_id=cid, has_side_effects=True, vmem_limit_bytes=62 * 2**20),
        name="gradient_sum",
    )(x, y, w_in, w_up, w_down)


SLOTS = 4
def upd_kernel(layers, eta, mu, x, y, gs, w_in, w_up, w_dn, m_in, m_up, m_dn,
               nw_in, nw_up, nw_dn, nm_in, nm_up, nm_dn, loss, h_out, wu, mu_, wd, md, g, h, p, a, ld_s, st_s):
    d, ff = w_up.shape[1:]
    d2, hf = d // 2, ff // 2
    steps = 4 + 2 * layers
    def where(s):
        v = jnp.maximum(s - 4, 0)
        return v // 2, lax.rem(v, 2)
    def moves(s, kind, put):
        sl = lax.rem(s, SLOTS)
        if kind == 0:
            at = pl.ds(pl.multiple_of(s * hf, hf), hf)
            arr = [((w_in, nw_in)[put].at[at], wd.at[sl]), ((m_in, nm_in)[put].at[at], md.at[sl])]
            gsrc, gdst = gs.at[pl.ds(2 * s, 2)], g.at[sl, pl.ds(0, 2)]
        else:
            l, j = where(s)
            at = pl.ds(pl.multiple_of(j * hf, hf), hf)
            arr = [((w_up, nw_up)[put].at[l, :, at], wu.at[sl]), ((m_up, nm_up)[put].at[l, :, at], mu_.at[sl]),
                   ((w_dn, nw_dn)[put].at[l, at], wd.at[sl]), ((m_dn, nm_dn)[put].at[l, at], md.at[sl])]
            gsrc, gdst = gs.at[pl.ds(8 + 8 * l + 4 * j, 4)], g.at[sl]
        if put:
            return [pltpu.make_async_copy(v, hb, st_s.at[sl, i]) for i, (hb, v) in enumerate(arr)]
        return [pltpu.make_async_copy(hb, v, ld_s.at[sl, i]) for i, (hb, v) in enumerate(arr)] + [pltpu.make_async_copy(gsrc, gdst, ld_s.at[sl, 4])]
    def go(s, put, what):
        @pl.when(jnp.logical_and(s >= 0, s < 4))
        def _():
            for c in moves(s, 0, put): getattr(c, what)()
        @pl.when(jnp.logical_and(s >= 4, s < steps))
        def _():
            for c in moves(s, 1, put): getattr(c, what)()
    for s in range(SLOTS - 1): go(jnp.int32(s), 0, "start")
    h[...] = jnp.zeros_like(h)
    def step(s, _):
        sl = lax.rem(s, SLOTS)
        go(s, 0, "wait")
        def upd(w, m, u, t, ix):
            nm = mu * m[(sl, *ix)] + g[sl, u, t].astype(f32)
            m[(sl, *ix)] = nm
            nw = w[(sl, *ix)] - eta * nm
            w[(sl, *ix)] = nw
            return nw.astype(bf)
        def down(lhs, u0):
            for j in range(2):
                cols = slice(j * d2, (j + 1) * d2)
                tot = h[:, cols]
                for t in range(2):
                    r = slice(t * hf // 2, (t + 1) * hf // 2)
                    tot = tot + dot(lhs(r), upd(wd, md, u0 + j, t, (r, cols)))
                h[:, cols] = tot
        @pl.when(s < 4)
        def _():
            xs = x[:, pl.ds(pl.multiple_of(s * hf, hf), hf)]
            down(lambda r: xs[:, r], 0)
        @pl.when(s >= 4)
        def _():
            @pl.when(lax.rem(s, 2) == 0)
            def _(): p[...] = h[...].astype(bf)
            for j in range(2):
                for t in range(2):
                    cols = slice(hf // 2 * j + d2 * t, hf // 2 * j + d2 * (t + 1))
                    a[:, cols] = gelu_tanh(dot(p[...], upd(wu, mu_, j, t, (slice(None), cols)))).astype(bf)
            down(lambda r: a[:, r], 2)
        go(s, 1, "start")
        go(s - 1, 1, "wait")
        go(s + SLOTS - 1, 0, "start")
        return 0
    lax.fori_loop(0, steps, step, 0)
    h_out[...] = h[...]
    e = h[...] - y[...].astype(f32)
    loss[...] = jnp.sum(e * e, axis=1) / (2 * d)
    go(jnp.int32(steps - 1), 1, "wait")

def update(eta, mu, x, y, g, w_in, w_up, w_down, m_in, m_up, m_down):
    rows = x.shape[0]
    layers, d, ff = w_up.shape
    vm = pl.BlockSpec(memory_space=pltpu.VMEM)
    hb = pl.BlockSpec(memory_space=pl.ANY)
    o = [jax.ShapeDtypeStruct(t.shape, f32) for t in (w_in, w_up, w_down, m_in, m_up, m_down)]
    o += [jax.ShapeDtypeStruct((rows,), f32), jax.ShapeDtypeStruct((rows, d), f32)]
    tile = [pltpu.VMEM((SLOTS, d, ff // 2), f32)] * 2 + [pltpu.VMEM((SLOTS, ff // 2, d), f32)] * 2
    return pl.pallas_call(
        functools.partial(upd_kernel, layers, eta, mu), out_shape=o,
        in_specs=[vm, vm] + [hb] * 7, out_specs=[hb] * 6 + [vm, vm],
        scratch_shapes=tile + [pltpu.VMEM((SLOTS, 4, 2, 512, d // 2), bf), pltpu.VMEM((rows, d), f32), pltpu.VMEM((rows, d), bf),
                               pltpu.VMEM((rows, ff // 2), bf), pltpu.SemaphoreType.DMA((SLOTS, 5)), pltpu.SemaphoreType.DMA((SLOTS, 4))],
        compiler_params=pltpu.CompilerParams(vmem_limit_bytes=63 * 2**20), name="update",
    )(x, y, g, w_in, w_up, w_down, m_in, m_up, m_down)


def solution(mesh):
    group_size = mesh.shape["data"]

    def device_steps(w_in, w_up, w_down, mom_in, mom_up, mom_down, x_now, y_now, x_next, y_next):
        local_rows, model_width = y_now.shape
        step_size = 4.0 * model_width / (w_up.shape[2] * (w_up.shape[0] + 1))
        total = gradient_sum(float(local_rows * group_size * model_width), x_now, y_now, w_in, w_up, w_down)
        out = update(step_size, MOMENTUM, x_next, y_next, total, w_in, w_up, w_down, mom_in, mom_up, mom_down)
        return tuple(out)

    row_spec = P("data", None)
    return jax.shard_map(
        device_steps,
        mesh=mesh,
        in_specs=(P(),) * 6 + (row_spec,) * 4,
        out_specs=(P(),) * 6 + (P("data"), row_spec),
        check_vma=False,
    )
```

```python
import functools

import jax
import jax.numpy as jnp
from jax import lax
from jax.experimental import pallas as pl
from jax.experimental.pallas import tpu as pltpu
from jax.sharding import PartitionSpec as P

MOMENTUM = 0.9
MESH = pl.DeviceIdType.MESH
BIT = {"c": 1, "x": 2, "y": 4, "a": 8, "b": 16}

bf, f32 = jnp.bfloat16, jnp.float32
TN = (((0,), (0,)), ((), ()))
NT = (((1,), (1,)), ((), ()))
def dot(a, b): return jnp.dot(a, b, preferred_element_type=f32)
def gelu_tanh(v): return jax.nn.gelu(v, approximate=True)

HOPS = {"mid": (0, "z", 1), "late": (0, 1, "z"), "early": ("z", 0, 1)}

def plan(types, tr, tw, K, KZ):
    sem, out = pltpu.SemaphoreType.DMA, []
    for ty in types:
        size = tr // 2
        for s, hop in enumerate(HOPS[ty]):
            if hop == "z":
                size //= 4
                out += [((ty, s, b), pltpu.VMEM((2, KZ, 3 * size, tw), bf)) for b in ("up", "down")]
                out += [((ty, s, b), sem((2, 2, KZ))) for b in ("rs", "rr", "as", "ar")]
            else:
                size //= 2
                out += [((ty, s, "buf"), pltpu.VMEM((2, K, size, tw), bf))]
                out += [((ty, s, b), sem((2, K))) for b in ("rs", "rr", "as", "ar")]
    return out

def grad_sum_kernel(layers, scale, nu, part, tr, tw, lags, kinds, names, *refs):
    (x_hbm, y, w_in, w_up, w_dn, gs, own_a, own_b, oth_a, oth_b, x, p_all, c_state, c_low, wup, wdn, w_s, x_s, g, acc, fin, rb0,
     c_s, c_r, d_s, d_r, st_s, h_s, h_r, hs_s) = refs[:30]
    mem = dict(zip(names, refs[30:]))
    types = sorted({n[0] for n in names})
    K, NS, NF = c_s.shape[0], acc.shape[0], fin.shape[0]
    KZ = [mem[n].shape[1] for n in names if n[2] == "up"][0]
    l0, lp, lz, ld = lags
    me = lax.axis_index("data")
    bit = {"c": lax.rem(me, 2), "x": lax.rem(me // 2, 2), "y": lax.rem(me // 4, 2)}
    peer = {d: me + w * (1 - 2 * bit[d]) for d, w in (("c", 1), ("x", 2), ("y", 4))}
    z = me // 8
    bar = pltpu.get_barrier_semaphore()
    def greet(dev):
        pl.semaphore_signal(bar, inc=1, device_id=(dev,), device_id_type=MESH)
    for d in "cxy":
        greet(peer[d])
    pl.when(z < 3)(lambda: greet(me + 8))
    pl.when(z > 0)(lambda: greet(me - 8))
    half, big = tr // 2, tr // 4
    DIMS = ("xy", "yx")
    o1 = l0
    def offsets(ty):
        zl = lz[ty]
        o4 = o1 + 2 * lp + 3 * zl
        o7 = 2 * o4 - o1
        return zl, o4, o7, o7 + ld
    o8 = max(offsets(ty)[3] for ty in types)
    assert NS >= max(offsets(ty)[1] for ty in types) and NF >= o8 - o1
    def rows(off, n):
        return pl.ds(pl.multiple_of(off, 16), n)
    def remote(src, dst, ss, rs, dev):
        return pltpu.make_async_remote_copy(src_ref=src, dst_ref=dst, send_sem=ss, recv_sem=rs, device_id=(dev,), device_id_type=MESH)
    def ix(u): return lax.rem(u, K)
    def iz(u): return lax.rem(u, KZ)
    def accr(u, off, n): return acc.at[lax.rem(u, NS), rows(off, n)]
    def finr(u, off, n): return fin.at[lax.rem(u, NF), rows(off, n)]
    def own(u): return lax.rem(u // 8, 2), lax.rem(u, 8)
    def out(u): return nu - 8 - 8 * (u // 8) + lax.rem(u, 8)
    def out_p(u): return part - 8 - 8 * (u // 8) + lax.rem(u, 8)
    def cp_c(u):
        return remote(g.at[(*own(u), 1 - bit["c"])], rb0.at[ix(u)], c_s.at[ix(u)], c_r.at[ix(u)], peer["c"])
    def cp_d(u):
        return remote(fin.at[lax.rem(u, NF)], gs.at[out(u), bit["c"]], d_s.at[ix(u)], d_r.at[ix(u)], peer["c"])
    def cp_st(u):
        return pltpu.make_async_copy(fin.at[lax.rem(u, NF)], gs.at[out(u), bit["c"]], st_s.at[ix(u)])
    home = [k * half + big * bit[DIMS[k][0]] for k in range(2)]
    def cp_h(u, k):
        return remote(finr(u, home[k], big), (oth_a, oth_b)[k].at[out_p(u)], h_s.at[k, ix(u)], h_r.at[k, ix(u)], peer["c"])
    def cp_hs(u, k):
        return pltpu.make_async_copy(finr(u, home[k], big), (own_a, own_b)[k].at[out_p(u)], hs_s.at[k, ix(u)])
    def add(dst, slot, r, a, b):
        dst[slot, r] = (a.astype(f32) + b.astype(f32)).astype(bf)
    snd_r = [lambda q: (q + 1, 3 - q), lambda q: (0, q)]
    rcv_r = [lambda q: (q, 4 - q), lambda q: (0, q + 1)]
    snd_a = [lambda q: (0, q + 1), lambda q: (q, 4 - q)]
    rcv_a = [lambda q: (0, q), lambda q: (q + 1, 3 - q)]
    senders, takers = [(0, 1, 2), (1, 2, 3)], [(1, 2, 3), (0, 1, 2)]
    def tick(t, _):
        def ev(off, f, cond=None):
            u = t - off
            ok = jnp.logical_and(u >= 0, u < nu)
            if cond is not None: ok = jnp.logical_and(ok, cond(u))
            pl.when(ok)(lambda: f(u))
        def whole(u): return u >= part
        def left(u): return u < part
        def e8(u):
            cp_d(u).wait(); cp_st(u).wait()
        def e8p(u):
            for k in range(2):
                cp_h(u, k).wait(); cp_hs(u, k).wait()
        def e7(u):
            cp_d(u).start(); cp_st(u).start()
        def e6p(u):
            for k in range(2):
                cp_h(u, k).start(); cp_hs(u, k).start()
        def e1(u):
            cp_c(u).wait()
            so, uo = own(u)
            for q in range(4):
                r = slice(q * big, (q + 1) * big)
                add(acc, lax.rem(u, NS), r, g[so, uo, bit["c"], r], rb0[ix(u), r])
        def line(ty, s, base, ch, o, lz, cond, gather, what):
            bufs, names_ = (mem[ty, s, "up"], mem[ty, s, "down"]), ("as", "ar") if gather else ("rs", "rr")
            snd, rcv = (snd_a, rcv_a) if gather else (snd_r, rcv_r)
            at = [o + z * lz, o + (3 - z) * lz]
            def cp(u, k, side, f, n):
                ss, rs = (mem[ty, s, m].at[side, k, iz(u)] for m in names_)
                r = (finr if gather else accr)(u, base[k] + ch * f, n * ch)
                return remote(r, r if gather else bufs[side].at[k, iz(u), pl.ds(0, n * ch)], ss, rs, me + (8, -8)[side])
            for side in range(2):
                if what == "arrive":
                    for q in senders[side]:
                        def sent(u, side=side, q=q):
                            for k in range(2): cp(u, k, side, *snd[side](q)).wait_send()
                        pl.when(z == q)(lambda: ev(at[side] + lz, sent, cond))
                    for q in takers[side]:
                        def got(u, side=side, q=q):
                            f, n = rcv[side](q)
                            for k in range(2):
                                cp(u, k, side, f, n).wait_recv()
                                if not gather:
                                    r = rows(base[k] + ch * f, n * ch)
                                    add(acc, lax.rem(u, NS), r, acc[lax.rem(u, NS), r], bufs[side][k, iz(u), 0:n * ch])
                        pl.when(z == q)(lambda: ev(at[side], got, cond))
                else:
                    for q in senders[side]:
                        def send(u, side=side, q=q):
                            for k in range(2): cp(u, k, side, *snd[side](q)).start()
                        pl.when(z == q)(lambda: ev(at[side], send, cond))
        def flow(ty):
            zl, o4, o7, o8 = offsets(ty)
            mine = lambda u: kinds(u, ty)
            mine_whole = lambda u: jnp.logical_and(mine(u), whole(u))
            ev(o8, e8, mine_whole)
            if part: ev(o7, e8p, lambda u: jnp.logical_and(mine(u), left(u)))
            base, size, hops = [[0, half]], [half], []
            o = o1
            for s, hop in enumerate(HOPS[ty]):
                if hop == "z":
                    n = size[-1] // 4
                    nb = [b + n * z for b in base[-1]]
                    give, dim = None, None
                    lag = 3 * zl
                else:
                    n = size[-1] // 2
                    dim = [DIMS[k][hop] for k in range(2)]
                    nb = [base[-1][k] + n * bit[dim[k]] for k in range(2)]
                    give = [base[-1][k] + n * (1 - bit[dim[k]]) for k in range(2)]
                    lag = lp
                hops.append((s, hop, base[-1], nb, n, give, dim, o, o + lag))
                base.append(nb); size.append(n)
                o += lag
            last_base, last = base[-1], size[-1]
            def pair_cp(u, k, s, src, dst, pre, dev):
                return remote(src, dst, mem[ty, s, pre + "s"].at[k, ix(u)], mem[ty, s, pre + "r"].at[k, ix(u)], peer[dev])
            o = o7
            for i, (s, hop, b, nb, n, give, dim, _, _) in enumerate(hops):
                cond = mine_whole if i == 0 else mine
                if hop == "z":
                    line(ty, s, b, n, o - 3 * zl, zl, cond, True, "arrive")
                else:
                    def arrive(u, s=s, nb=nb, n=n, dim=dim):
                        for k in range(2): pair_cp(u, k, s, finr(u, nb[k], n), finr(u, nb[k], n), "a", dim[k]).wait()
                    ev(o, arrive, cond)
                if i == 0:
                    ev(o7, e7, mine_whole)
                else:
                    depart_g(*prev)
                    if i == 1 and part: ev(o, e6p, lambda u: jnp.logical_and(mine(u), left(u)))
                def depart_g(s, hop, b, nb, n, dim, o, cond):
                    if hop == "z":
                        line(ty, s, b, n, o, zl, cond, True, "depart")
                    else:
                        def go(u):
                            for k in range(2): pair_cp(u, k, s, finr(u, nb[k], n), finr(u, nb[k], n), "a", dim[k]).start()
                        ev(o, go, cond)
                o -= 3 * zl if hop == "z" else lp
                prev = (s, hop, b, nb, n, dim, o, cond)
            for i, (s, hop, b, nb, n, give, dim, oa, ob) in reversed(list(enumerate(hops))):
                if hop == "z":
                    line(ty, s, b, n, oa, zl, mine, False, "arrive")
                else:
                    def arrive(u, s=s, nb=nb, n=n, give=give, dim=dim):
                        for k in range(2):
                            pair_cp(u, k, s, accr(u, give[k], n), mem[ty, s, "buf"].at[k, ix(u)], "r", dim[k]).wait()
                            r = rows(nb[k], n)
                            add(acc, lax.rem(u, NS), r, acc[lax.rem(u, NS), r], mem[ty, s, "buf"][k, ix(u)])
                    ev(ob, arrive, mine)
                if i == len(hops) - 1:
                    def finish(u):
                        for k in range(2):
                            r = rows(last_base[k], last)
                            fin[lax.rem(u, NF), r] = acc[lax.rem(u, NS), r]
                    ev(o4, finish, mine)
                    depart_g(*prev)
                else:
                    depart_r(*prev_r)
                def depart_r(s, hop, b, n, give, dim, oa):
                    if hop == "z":
                        line(ty, s, b, n, oa, zl, mine, False, "depart")
                    else:
                        def go(u):
                            for k in range(2): pair_cp(u, k, s, accr(u, give[k], n), mem[ty, s, "buf"].at[k, ix(u)], "r", dim[k]).start()
                        ev(oa, go, mine)
                prev_r = (s, hop, b, n, give, dim, oa)
            return depart_r, prev_r
        firsts = [flow(ty) for ty in types]
        ev(o1, e1)
        for f, args in firsts: f(*args)
        ev(0, lambda u: cp_c(u).start())
        return 0
    d, ff = w_up.shape[1:]
    def cp_w(layer, k):
        sl = lax.rem(layer, 2)
        src, dst = ((w_up, wup), (w_dn, wdn))[k]
        return pltpu.make_async_copy(src.at[layer], dst.at[sl], w_s.at[k, sl])
    e4 = w_in.shape[0] // 4
    cp_x = pltpu.make_async_copy(x_hbm, x, x_s.at[4])
    cp_in = [pltpu.make_async_copy(w_in.at[pl.ds(i * e4, e4)], wdn.at[i // 2, pl.ds((i % 2) * e4, e4)], x_s.at[i]) for i in range(4)]
    cp_x.start()
    for c in cp_in: c.start()
    for l in range(2): cp_w(l, 0).start()
    cp_x.wait()
    h = c_state
    for i in range(4):
        cp_in[i].wait()
        piece = dot(x[:, i * e4:(i + 1) * e4], wdn[i // 2, (i % 2) * e4:(i % 2 + 1) * e4].astype(bf))
        h[...] = piece if i == 0 else h[...] + piece
        if i % 2 == 1: cp_w(i // 2, 1).start()
    n = ff // 4
    def layer_fwd(l, _):
        sl = lax.rem(l, 2)
        pin = h[...].astype(bf)
        p_all[l] = pin
        tot = h[...]
        cp_w(l, 0).wait()
        acts = [gelu_tanh(dot(pin, wup[sl, :, q * n:(q + 1) * n].astype(bf))).astype(bf) for q in range(4)]
        cp_w(l, 1).wait()
        for q in range(4):
            tot = tot + dot(acts[q], wdn[sl, q * n:(q + 1) * n].astype(bf))
        h[...] = tot
        @pl.when(l < layers - 2)
        def _():
            for k in range(2): cp_w(l + 2, k).start()
        return 0
    lax.fori_loop(0, layers, layer_fwd, 0)
    c_state[...] = (h[...] - y[...].astype(f32)) / scale
    pl.semaphore_wait(bar, 3 + jnp.minimum(z, 1) + jnp.minimum(3 - z, 1))
    d2 = d // 2
    def chunk(step, q):
        gl = lax.rem(step, 2)
        layer = layers - 1 - step
        sl = lax.rem(layer, 2)
        @pl.when(jnp.logical_and(q == 0, step <= layers))
        def _():
            c_low[...] = c_state[...].astype(bf)
        @pl.when(jnp.logical_and(q == 0, jnp.logical_and(step >= 2, step < layers)))
        def _():
            for k in range(2): cp_w(layer, k).wait()
        @pl.when(jnp.logical_and(q == 0, jnp.logical_and(step >= 1, step < layers - 1)))
        def _():
            for k in range(2): cp_w(layer - 1, k).start()
        @pl.when(step < layers)
        def _():
            cols = pl.ds(pl.multiple_of(q * n, n), n)
            pin = p_all[layer]
            wu = wup[sl, :, cols].astype(bf)
            act, back = jax.vjp(gelu_tanh, dot(pin, wu))
            ac = lax.dot_general(c_low[...], wdn[sl, cols, :].astype(bf), NT, preferred_element_type=f32)
            pre = back(ac)[0].astype(bf)
            gd = lax.dot_general(act.astype(bf), c_low[...], TN, preferred_element_type=f32).astype(bf)
            gu = lax.dot_general(pin, pre, TN, preferred_element_type=f32).astype(bf)
            for t in range(2):
                g[gl, 4 * (q // 2) + lax.rem(q, 2), t] = gu[:, t * d2:(t + 1) * d2]
                g[gl, 4 * (q // 2) + 2 + t, lax.rem(q, 2)] = gd[:, t * d2:(t + 1) * d2]
            c_state[...] += lax.dot_general(pre, wu, NT, preferred_element_type=f32)
        @pl.when(step == layers)
        def _():
            for r in range(2):
                xs = x[:, pl.ds(pl.multiple_of((2 * q + r) * tr, tr), tr)]
                gi = lax.dot_general(xs, c_low[...], TN, preferred_element_type=f32).astype(bf)
                for t in range(2):
                    g[gl, 2 * q + t, r] = gi[:, t * d2:(t + 1) * d2]
    def block(b, _):
        lax.fori_loop(2 * b - 4, 2 * b - 2, tick, 0)
        chunk(b // 4, lax.rem(b, 4))
        return 0
    lax.fori_loop(0, 2 + (nu + o8 + 1) // 2, block, 0)

def gradient_sum(scale, x, y, w_in, w_up, w_down, part, kinds, types, lags=(1, 2, {"mid": 2, "late": 2, "early": 4}, 1), cid=0, K=8, KZ=8, NS=16, NF=32):
    layers, d, ff = w_up.shape
    rows = x.shape[0]
    nu, tr, tw = 8 * (layers + 1), 512, d // 2
    l0, lp, lz, ld = lags
    vm = pl.BlockSpec(memory_space=pltpu.VMEM)
    hb = pl.BlockSpec(memory_space=pl.ANY)
    sem = pltpu.SemaphoreType.DMA
    hops = plan(types, tr, tw, K, KZ)
    left = jax.ShapeDtypeStruct((max(part, 8), tr // 4, tw), bf)
    return pl.pallas_call(
        functools.partial(grad_sum_kernel, layers, scale, nu, part, tr, tw, lags, kinds, [n for n, _ in hops]),
        out_shape=[jax.ShapeDtypeStruct((nu - part, 2, tr, tw), bf)] + [left] * 4,
        in_specs=[hb, vm, hb, hb, hb],
        out_specs=[hb] * 5,
        scratch_shapes=[pltpu.VMEM(x.shape, bf), pltpu.VMEM((layers, rows, d), bf), pltpu.VMEM((rows, d), f32), pltpu.VMEM((rows, d), bf),
                        pltpu.VMEM((2, d, ff), f32), pltpu.VMEM((2, ff, d), f32), sem((2, 2)), sem((5,)), pltpu.VMEM((2, 8, 2, tr, tw), bf),
                        pltpu.VMEM((NS, tr, tw), bf), pltpu.VMEM((NF, tr, tw), bf), pltpu.VMEM((K, tr, tw), bf)]
        + [sem((K,))] * 5 + [sem((2, K))] * 3 + [spec for _, spec in hops],
        compiler_params=pltpu.CompilerParams(collective_id=cid, has_side_effects=True, vmem_limit_bytes=63 * 2**20),
        name="gradient_sum",
    )(x, y, w_in, w_up, w_down)


SLOTS = 4
def upd_kernel(layers, lo, hi, eta, mu, *refs):
    scratch = refs[-11:]
    wu, mu_, wd, md, g, h, p, a, ld_s, st_s, g_s = scratch
    first, last = lo == 0, hi == layers
    if first:
        x, gs, w_in, w_up, w_dn, m_in, m_up, m_dn, nw_in, nw_up, nw_dn, nm_in, nm_up, nm_dn, h_out = refs[:-11]
    elif last:
        y, h_in, *pieces = refs[:10]
        w_up, w_dn, m_up, m_dn, _, _, _, _, nw_up, nw_dn, nm_up, nm_dn, loss, h_out = refs[10:-11]
    else:
        h_in, gs, w_up, w_dn, m_up, m_dn, _, _, _, _, nw_up, nw_dn, nm_up, nm_dn, h_out = refs[:-11]
    d, ff = w_up.shape[1:]
    d2, hf = d // 2, ff // 2
    ins = 4 if first else 0
    steps = ins + 2 * (hi - lo)
    def where(s):
        v = jnp.maximum(s - ins, 0)
        return lo + v // 2, lax.rem(v, 2)
    def moves(s, group, put):
        sl = lax.rem(s, SLOTS)
        if group == "in":
            at = pl.ds(pl.multiple_of(s * hf, hf), hf)
            arr = [((w_in, nw_in)[put].at[at], wd.at[sl]), ((m_in, nm_in)[put].at[at], md.at[sl])]
        else:
            l, j = where(s)
            at = pl.ds(pl.multiple_of(j * hf, hf), hf)
            if group == "up":
                arr = [((w_up, nw_up)[put].at[l, :, at], wu.at[sl]), ((m_up, nm_up)[put].at[l, :, at], mu_.at[sl])]
            else:
                arr = [((w_dn, nw_dn)[put].at[l, at], wd.at[sl]), ((m_dn, nm_dn)[put].at[l, at], md.at[sl])]
        o = 0 if group == "up" else 2
        sems = (ld_s, st_s)[put]
        return [pltpu.make_async_copy(*((v, hb) if put else (hb, v)), sems.at[sl, o + i]) for i, (hb, v) in enumerate(arr)]
    def grads(s, kind, what):
        sl = lax.rem(s, SLOTS)
        if kind == "in":
            c = pltpu.make_async_copy(gs.at[pl.ds(2 * s, 2)], g.at[sl, pl.ds(0, 2)], g_s.at[sl, 0])
            return getattr(c, what)()
        l, j = where(s)
        if not last:
            c = pltpu.make_async_copy(gs.at[pl.ds(8 + 8 * l + 4 * j, 4)], g.at[sl], g_s.at[sl, 0])
            return getattr(c, what)()
        me = lax.axis_index("data")
        c, q = lax.rem(me, 2), 128
        at = 8 * (l - lo) + 4 * j
        for k in range(2):
            b = lax.rem(me // (2, 4)[k], 2)
            for i in range(4):
                row = pl.multiple_of(256 * k + q * (b if i < 2 else 1 - b), q)
                half = c if i % 2 == 0 else 1 - c
                cp = pltpu.make_async_copy(pieces[4 * k + i].at[pl.ds(at, 4)], g.at[sl, :, half, pl.ds(row, q)], g_s.at[sl, 4 * k + i])
                getattr(cp, what)()
    def on(s, kind, f):
        if kind == "in":
            if first: pl.when(jnp.logical_and(s >= 0, s < ins))(f)
        else:
            pl.when(jnp.logical_and(s >= ins, s < steps))(f)
    def load(s):
        def go_in():
            grads(s, "in", "start")
            for c in moves(s, "in", 0): c.start()
        def go():
            grads(s, "layer", "start")
            for c in moves(s, "up", 0) + moves(s, "down", 0): c.start()
        on(s, "in", go_in); on(s, "layer", go)
    def stored(s):
        def go_in():
            for c in moves(s, "in", 1): c.wait()
        def go():
            for c in moves(s, "up", 1) + moves(s, "down", 1): c.wait()
        on(s, "in", go_in); on(s, "layer", go)
    for s in range(SLOTS - 1): load(jnp.int32(s))
    h[...] = jnp.zeros_like(h) if first else h_in[...]
    def step(s, _):
        sl = lax.rem(s, SLOTS)
        def upd(w, m, u, t, ix):
            nm = mu * m[(sl, *ix)] + g[sl, u, t].astype(f32)
            m[(sl, *ix)] = nm
            nw = w[(sl, *ix)] - eta * nm
            w[(sl, *ix)] = nw
            return nw.astype(bf)
        def down(lhs, u0):
            for j in range(2):
                cols = slice(j * d2, (j + 1) * d2)
                tot = h[:, cols]
                for t in range(2):
                    r = slice(t * hf // 2, (t + 1) * hf // 2)
                    tot = tot + dot(lhs(r), upd(wd, md, u0 + j, t, (r, cols)))
                h[:, cols] = tot
        def do_in():
            grads(s, "in", "wait")
            for c in moves(s, "in", 0): c.wait()
            xs = x[:, pl.ds(pl.multiple_of(s * hf, hf), hf)]
            down(lambda r: xs[:, r], 0)
            for c in moves(s, "in", 1): c.start()
        def do_layer():
            grads(s, "layer", "wait")
            for c in moves(s, "up", 0): c.wait()
            @pl.when(where(s)[1] == 0)
            def _(): p[...] = h[...].astype(bf)
            for j in range(2):
                for t in range(2):
                    cols = slice(hf // 2 * j + d2 * t, hf // 2 * j + d2 * (t + 1))
                    a[:, cols] = gelu_tanh(dot(p[...], upd(wu, mu_, j, t, (slice(None), cols)))).astype(bf)
            for c in moves(s, "up", 1): c.start()
            for c in moves(s, "down", 0): c.wait()
            down(lambda r: a[:, r], 2)
            for c in moves(s, "down", 1): c.start()
        on(s, "in", do_in); on(s, "layer", do_layer)
        stored(s - 1)
        load(s + SLOTS - 1)
        return 0
    lax.fori_loop(0, steps, step, 0)
    h_out[...] = h[...]
    if last:
        e = h[...] - y[...].astype(f32)
        loss[...] = jnp.sum(e * e, axis=1) / (2 * d)
    stored(jnp.int32(steps - 1))

def flip(v, mask, n):
    return lax.ppermute(v, "data", [(i, i ^ mask) for i in range(n)])

def update(eta, mu, x, y, g, halves, w_in, w_up, w_down, m_in, m_up, m_down, n):
    rows = x.shape[0]
    layers, d, ff = w_up.shape
    own_a, own_b, oth_a, oth_b = halves
    mid = layers - own_a.shape[0] // 8
    vm = pl.BlockSpec(memory_space=pltpu.VMEM)
    hb = pl.BlockSpec(memory_space=pl.ANY)
    sem = pltpu.SemaphoreType.DMA
    scratch = [pltpu.VMEM((SLOTS, d, ff // 2), f32)] * 2 + [pltpu.VMEM((SLOTS, ff // 2, d), f32)] * 2
    scratch += [pltpu.VMEM((SLOTS, 4, 2, 512, d // 2), bf), pltpu.VMEM((rows, d), f32), pltpu.VMEM((rows, d), bf),
                pltpu.VMEM((rows, ff // 2), bf), sem((SLOTS, 4)), sem((SLOTS, 4)), sem((SLOTS, 8))]
    params = pltpu.CompilerParams(vmem_limit_bytes=60 * 2**20)
    h_type = jax.ShapeDtypeStruct((rows, d), f32)
    def call(lo, hi, outs, ins, specs, aliases):
        c = (8 * (hi - lo) + 8 * (lo == 0)) * 512 * d
        return pl.pallas_call(
            functools.partial(upd_kernel, layers, lo, hi, eta, mu), out_shape=outs, in_specs=specs,
            out_specs=[hb if len(t.shape) > 2 or t.shape[0] > rows else vm for t in outs], scratch_shapes=scratch, compiler_params=params,
            input_output_aliases=aliases, cost_estimate=pl.CostEstimate(flops=4 * rows * c, bytes_accessed=18 * c, transcendentals=0),
            name="update_" + str(lo),
        )(*ins)
    o = [jax.ShapeDtypeStruct(t.shape, f32) for t in (w_in, w_up, w_down, m_in, m_up, m_down)]
    cut = mid - 1
    ax, bx = flip(own_a, 2, n), flip(own_b, 4, n)
    nw_in, nw_up, nw_dn, nm_in, nm_up, nm_dn, h = call(
        0, cut, o + [h_type], (x, g, w_in, w_up, w_down, m_in, m_up, m_down), [vm] + [hb] * 7, {})
    h, ax, bx = lax.optimization_barrier((h, ax, bx))
    ac, bc = flip(ax, 1, n), flip(bx, 1, n)
    mats = [o[1], o[2], o[4], o[5]]
    nw_up, nw_dn, nm_up, nm_dn, h = call(
        cut, mid, mats + [h_type], (h, g, w_up, w_down, m_up, m_down, nw_up, nw_dn, nm_up, nm_dn), [vm] + [hb] * 9,
        {6: 0, 7: 1, 8: 2, 9: 3})
    nw_up, nw_dn, nm_up, nm_dn, loss, h = call(
        mid, layers, mats + [jax.ShapeDtypeStruct((rows,), f32), h_type],
        (y, h, own_a, oth_a, ax, ac, own_b, oth_b, bx, bc, w_up, w_down, m_up, m_down, nw_up, nw_dn, nm_up, nm_dn), [vm, vm] + [hb] * 16,
        {14: 0, 15: 1, 16: 2, 17: 3})
    return nw_in, nw_up, nw_dn, nm_in, nm_up, nm_dn, loss, h

PERMUTED_LAYERS = 6

def solution(mesh):
    group_size = mesh.shape["data"]

    def device_steps(w_in, w_up, w_down, mom_in, mom_up, mom_down, x_now, y_now, x_next, y_next):
        local_rows, model_width = y_now.shape
        step_size = 4.0 * model_width / (w_up.shape[2] * (w_up.shape[0] + 1))
        part = 8 * PERMUTED_LAYERS
        def kinds(u, ty):
            odd = lax.rem(u, 2) == 1
            if ty == "late":
                return jnp.logical_and(u < part, odd)
            return jnp.logical_or(u >= part, jnp.logical_not(odd))
        total, own_a, own_b, oth_a, oth_b = gradient_sum(
            float(local_rows * group_size * model_width), x_now, y_now, w_in, w_up, w_down, part, kinds, ("late", "mid"))
        return update(step_size, MOMENTUM, x_next, y_next, total, (own_a, own_b, oth_a, oth_b), w_in, w_up, w_down, mom_in, mom_up, mom_down, group_size)

    row_spec = P("data", None)
    return jax.shard_map(
        device_steps,
        mesh=mesh,
        in_specs=(P(),) * 6 + (row_spec,) * 4,
        out_specs=(P(),) * 6 + (P("data"), row_spec),
        check_vma=False,
    )
```

```python
import functools

import jax
import jax.numpy as jnp
from jax import lax
from jax.experimental import pallas as pl
from jax.experimental.pallas import tpu as pltpu
from jax.sharding import PartitionSpec as P

MOMENTUM = 0.9
MESH = pl.DeviceIdType.MESH
BIT = {"c": 1, "x": 2, "y": 4, "a": 8, "b": 16}

bf, f32 = jnp.bfloat16, jnp.float32
TN = (((0,), (0,)), ((), ()))
NT = (((1,), (1,)), ((), ()))
def dot(a, b): return jnp.dot(a, b, preferred_element_type=f32)
def gelu_tanh(v): return jax.nn.gelu(v, approximate=True)

HOPS = {"mid": (0, "z", 1), "late": (0, 1, "z"), "early": ("z", 0, 1)}

def plan(types, tr, tw, K, KZ):
    sem, out = pltpu.SemaphoreType.DMA, []
    for ty in types:
        size = tr // 2
        for s, hop in enumerate(HOPS[ty]):
            if hop == "z":
                size //= 4
                out += [((ty, s, b), pltpu.VMEM((2, KZ, 3 * size, tw), bf)) for b in ("up", "down")]
                out += [((ty, s, b), sem((2, 2, KZ))) for b in ("rs", "rr", "as", "ar")]
            else:
                size //= 2
                out += [((ty, s, "buf"), pltpu.VMEM((2, K, size, tw), bf))]
                out += [((ty, s, b), sem((2, K))) for b in ("rs", "rr", "as", "ar")]
    return out

def grad_sum_kernel(layers, scale, nu, part, tr, tw, lags, kinds, names, *refs):
    (x_hbm, y, w_in, w_up, w_dn, gs, own_a, own_b, oth_a, oth_b, x, p_all, c_state, c_low, wup, wdn, w_s, x_s, g, acc, fin, rb0,
     c_s, c_r, d_s, d_r, st_s, h_s, h_r, hs_s) = refs[:30]
    mem = dict(zip(names, refs[30:]))
    types = sorted({n[0] for n in names})
    K, NS, NF = c_s.shape[0], acc.shape[0], fin.shape[0]
    KZ = [mem[n].shape[1] for n in names if n[2] == "up"][0]
    l0, lp, lz, ld = lags
    me = lax.axis_index("data")
    bit = {"c": lax.rem(me, 2), "x": lax.rem(me // 2, 2), "y": lax.rem(me // 4, 2)}
    peer = {d: me + w * (1 - 2 * bit[d]) for d, w in (("c", 1), ("x", 2), ("y", 4))}
    z = me // 8
    bar = pltpu.get_barrier_semaphore()
    def greet(dev):
        pl.semaphore_signal(bar, inc=1, device_id=(dev,), device_id_type=MESH)
    for d in "cxy":
        greet(peer[d])
    pl.when(z < 3)(lambda: greet(me + 8))
    pl.when(z > 0)(lambda: greet(me - 8))
    half, big = tr // 2, tr // 4
    DIMS = ("xy", "yx")
    o1 = l0
    def offsets(ty):
        zl = lz[ty]
        o4 = o1 + 2 * lp + 3 * zl
        o7 = 2 * o4 - o1
        return zl, o4, o7, o7 + ld
    o8 = max(offsets(ty)[3] for ty in types)
    assert NS >= max(offsets(ty)[1] for ty in types) and NF >= o8 - o1
    def rows(off, n):
        return pl.ds(pl.multiple_of(off, 16), n)
    def remote(src, dst, ss, rs, dev):
        return pltpu.make_async_remote_copy(src_ref=src, dst_ref=dst, send_sem=ss, recv_sem=rs, device_id=(dev,), device_id_type=MESH)
    def ix(u): return lax.rem(u, K)
    def iz(u): return lax.rem(u, KZ)
    def accr(u, off, n): return acc.at[lax.rem(u, NS), rows(off, n)]
    def finr(u, off, n): return fin.at[lax.rem(u, NF), rows(off, n)]
    def own(u): return lax.rem(u // 8, 2), lax.rem(u, 8)
    def out(u): return nu - 8 - 8 * (u // 8) + lax.rem(u, 8)
    def out_p(u): return part - 8 - 8 * (u // 8) + lax.rem(u, 8)
    def cp_c(u):
        return remote(g.at[(*own(u), 1 - bit["c"])], rb0.at[ix(u)], c_s.at[ix(u)], c_r.at[ix(u)], peer["c"])
    def cp_d(u):
        return remote(fin.at[lax.rem(u, NF)], gs.at[out(u), bit["c"]], d_s.at[ix(u)], d_r.at[ix(u)], peer["c"])
    def cp_st(u):
        return pltpu.make_async_copy(fin.at[lax.rem(u, NF)], gs.at[out(u), bit["c"]], st_s.at[ix(u)])
    home = [k * half + big * bit[DIMS[k][0]] for k in range(2)]
    def cp_h(u, k):
        return remote(finr(u, home[k], big), (oth_a, oth_b)[k].at[out_p(u)], h_s.at[k, ix(u)], h_r.at[k, ix(u)], peer["c"])
    def cp_hs(u, k):
        return pltpu.make_async_copy(finr(u, home[k], big), (own_a, own_b)[k].at[out_p(u)], hs_s.at[k, ix(u)])
    def add(dst, slot, r, a, b):
        dst[slot, r] = (a.astype(f32) + b.astype(f32)).astype(bf)
    snd_r = [lambda q: (q + 1, 3 - q), lambda q: (0, q)]
    rcv_r = [lambda q: (q, 4 - q), lambda q: (0, q + 1)]
    snd_a = [lambda q: (0, q + 1), lambda q: (q, 4 - q)]
    rcv_a = [lambda q: (0, q), lambda q: (q + 1, 3 - q)]
    senders, takers = [(0, 1, 2), (1, 2, 3)], [(1, 2, 3), (0, 1, 2)]
    def tick(t, _):
        def ev(off, f, cond=None):
            u = t - off
            ok = jnp.logical_and(u >= 0, u < nu)
            if cond is not None: ok = jnp.logical_and(ok, cond(u))
            pl.when(ok)(lambda: f(u))
        def whole(u): return u >= part
        def left(u): return u < part
        def e8(u):
            cp_d(u).wait(); cp_st(u).wait()
        def e8p(u):
            for k in range(2):
                cp_h(u, k).wait(); cp_hs(u, k).wait()
        def e7(u):
            cp_d(u).start(); cp_st(u).start()
        def e6p(u):
            for k in range(2):
                cp_h(u, k).start(); cp_hs(u, k).start()
        def e1(u):
            cp_c(u).wait()
            so, uo = own(u)
            for q in range(4):
                r = slice(q * big, (q + 1) * big)
                add(acc, lax.rem(u, NS), r, g[so, uo, bit["c"], r], rb0[ix(u), r])
        def line(ty, s, base, ch, o, lz, cond, gather, what):
            bufs, names_ = (mem[ty, s, "up"], mem[ty, s, "down"]), ("as", "ar") if gather else ("rs", "rr")
            snd, rcv = (snd_a, rcv_a) if gather else (snd_r, rcv_r)
            at = [o + z * lz, o + (3 - z) * lz]
            def cp(u, k, side, f, n):
                ss, rs = (mem[ty, s, m].at[side, k, iz(u)] for m in names_)
                r = (finr if gather else accr)(u, base[k] + ch * f, n * ch)
                return remote(r, r if gather else bufs[side].at[k, iz(u), pl.ds(0, n * ch)], ss, rs, me + (8, -8)[side])
            for side in range(2):
                if what == "arrive":
                    for q in senders[side]:
                        def sent(u, side=side, q=q):
                            for k in range(2): cp(u, k, side, *snd[side](q)).wait_send()
                        pl.when(z == q)(lambda: ev(at[side] + lz, sent, cond))
                    for q in takers[side]:
                        def got(u, side=side, q=q):
                            f, n = rcv[side](q)
                            for k in range(2):
                                cp(u, k, side, f, n).wait_recv()
                                if not gather:
                                    r = rows(base[k] + ch * f, n * ch)
                                    add(acc, lax.rem(u, NS), r, acc[lax.rem(u, NS), r], bufs[side][k, iz(u), 0:n * ch])
                        pl.when(z == q)(lambda: ev(at[side], got, cond))
                else:
                    for q in senders[side]:
                        def send(u, side=side, q=q):
                            for k in range(2): cp(u, k, side, *snd[side](q)).start()
                        pl.when(z == q)(lambda: ev(at[side], send, cond))
        def flow(ty):
            zl, o4, o7, o8 = offsets(ty)
            mine = lambda u: kinds(u, ty)
            mine_whole = lambda u: jnp.logical_and(mine(u), whole(u))
            ev(o8, e8, mine_whole)
            if part: ev(o7, e8p, lambda u: jnp.logical_and(mine(u), left(u)))
            base, size, hops = [[0, half]], [half], []
            o = o1
            for s, hop in enumerate(HOPS[ty]):
                if hop == "z":
                    n = size[-1] // 4
                    nb = [b + n * z for b in base[-1]]
                    give, dim = None, None
                    lag = 3 * zl
                else:
                    n = size[-1] // 2
                    dim = [DIMS[k][hop] for k in range(2)]
                    nb = [base[-1][k] + n * bit[dim[k]] for k in range(2)]
                    give = [base[-1][k] + n * (1 - bit[dim[k]]) for k in range(2)]
                    lag = lp
                hops.append((s, hop, base[-1], nb, n, give, dim, o, o + lag))
                base.append(nb); size.append(n)
                o += lag
            last_base, last = base[-1], size[-1]
            def pair_cp(u, k, s, src, dst, pre, dev):
                return remote(src, dst, mem[ty, s, pre + "s"].at[k, ix(u)], mem[ty, s, pre + "r"].at[k, ix(u)], peer[dev])
            o = o7
            for i, (s, hop, b, nb, n, give, dim, _, _) in enumerate(hops):
                cond = mine_whole if i == 0 else mine
                if hop == "z":
                    line(ty, s, b, n, o - 3 * zl, zl, cond, True, "arrive")
                else:
                    def arrive(u, s=s, nb=nb, n=n, dim=dim):
                        for k in range(2): pair_cp(u, k, s, finr(u, nb[k], n), finr(u, nb[k], n), "a", dim[k]).wait()
                    ev(o, arrive, cond)
                if i == 0:
                    ev(o7, e7, mine_whole)
                else:
                    depart_g(*prev)
                    if i == 1 and part: ev(o, e6p, lambda u: jnp.logical_and(mine(u), left(u)))
                def depart_g(s, hop, b, nb, n, dim, o, cond):
                    if hop == "z":
                        line(ty, s, b, n, o, zl, cond, True, "depart")
                    else:
                        def go(u):
                            for k in range(2): pair_cp(u, k, s, finr(u, nb[k], n), finr(u, nb[k], n), "a", dim[k]).start()
                        ev(o, go, cond)
                o -= 3 * zl if hop == "z" else lp
                prev = (s, hop, b, nb, n, dim, o, cond)
            for i, (s, hop, b, nb, n, give, dim, oa, ob) in reversed(list(enumerate(hops))):
                if hop == "z":
                    line(ty, s, b, n, oa, zl, mine, False, "arrive")
                else:
                    def arrive(u, s=s, nb=nb, n=n, give=give, dim=dim):
                        for k in range(2):
                            pair_cp(u, k, s, accr(u, give[k], n), mem[ty, s, "buf"].at[k, ix(u)], "r", dim[k]).wait()
                            r = rows(nb[k], n)
                            add(acc, lax.rem(u, NS), r, acc[lax.rem(u, NS), r], mem[ty, s, "buf"][k, ix(u)])
                    ev(ob, arrive, mine)
                if i == len(hops) - 1:
                    def finish(u):
                        for k in range(2):
                            r = rows(last_base[k], last)
                            fin[lax.rem(u, NF), r] = acc[lax.rem(u, NS), r]
                    ev(o4, finish, mine)
                    depart_g(*prev)
                else:
                    depart_r(*prev_r)
                def depart_r(s, hop, b, n, give, dim, oa):
                    if hop == "z":
                        line(ty, s, b, n, oa, zl, mine, False, "depart")
                    else:
                        def go(u):
                            for k in range(2): pair_cp(u, k, s, accr(u, give[k], n), mem[ty, s, "buf"].at[k, ix(u)], "r", dim[k]).start()
                        ev(oa, go, mine)
                prev_r = (s, hop, b, n, give, dim, oa)
            return depart_r, prev_r
        firsts = [flow(ty) for ty in types]
        ev(o1, e1)
        for f, args in firsts: f(*args)
        ev(0, lambda u: cp_c(u).start())
        return 0
    d, ff = w_up.shape[1:]
    def cp_w(layer, k):
        sl = lax.rem(layer, 2)
        src, dst = ((w_up, wup), (w_dn, wdn))[k]
        return pltpu.make_async_copy(src.at[layer], dst.at[sl], w_s.at[k, sl])
    e4 = w_in.shape[0] // 4
    cp_x = pltpu.make_async_copy(x_hbm, x, x_s.at[4])
    cp_in = [pltpu.make_async_copy(w_in.at[pl.ds(i * e4, e4)], wdn.at[i // 2, pl.ds((i % 2) * e4, e4)], x_s.at[i]) for i in range(4)]
    cp_x.start()
    for c in cp_in: c.start()
    for l in range(2): cp_w(l, 0).start()
    cp_x.wait()
    h = c_state
    for i in range(4):
        cp_in[i].wait()
        piece = dot(x[:, i * e4:(i + 1) * e4], wdn[i // 2, (i % 2) * e4:(i % 2 + 1) * e4].astype(bf))
        h[...] = piece if i == 0 else h[...] + piece
        if i % 2 == 1: cp_w(i // 2, 1).start()
    n = ff // 4
    def layer_fwd(l, _):
        sl = lax.rem(l, 2)
        pin = h[...].astype(bf)
        p_all[l] = pin
        tot = h[...]
        cp_w(l, 0).wait()
        acts = [gelu_tanh(dot(pin, wup[sl, :, q * n:(q + 1) * n].astype(bf))).astype(bf) for q in range(4)]
        cp_w(l, 1).wait()
        for q in range(4):
            tot = tot + dot(acts[q], wdn[sl, q * n:(q + 1) * n].astype(bf))
        h[...] = tot
        @pl.when(l < layers - 2)
        def _():
            for k in range(2): cp_w(l + 2, k).start()
        return 0
    lax.fori_loop(0, layers, layer_fwd, 0)
    c_state[...] = (h[...] - y[...].astype(f32)) / scale
    pl.semaphore_wait(bar, 3 + jnp.minimum(z, 1) + jnp.minimum(3 - z, 1))
    d2 = d // 2
    def chunk(step, q):
        gl = lax.rem(step, 2)
        layer = layers - 1 - step
        sl = lax.rem(layer, 2)
        @pl.when(jnp.logical_and(q == 0, step <= layers))
        def _():
            c_low[...] = c_state[...].astype(bf)
        @pl.when(jnp.logical_and(q == 0, jnp.logical_and(step >= 2, step < layers)))
        def _():
            for k in range(2): cp_w(layer, k).wait()
        @pl.when(jnp.logical_and(q == 0, jnp.logical_and(step >= 1, step < layers - 1)))
        def _():
            for k in range(2): cp_w(layer - 1, k).start()
        @pl.when(step < layers)
        def _():
            cols = pl.ds(pl.multiple_of(q * n, n), n)
            pin = p_all[layer]
            wu = wup[sl, :, cols].astype(bf)
            act, back = jax.vjp(gelu_tanh, dot(pin, wu))
            ac = lax.dot_general(c_low[...], wdn[sl, cols, :].astype(bf), NT, preferred_element_type=f32)
            pre = back(ac)[0].astype(bf)
            gd = lax.dot_general(act.astype(bf), c_low[...], TN, preferred_element_type=f32).astype(bf)
            gu = lax.dot_general(pin, pre, TN, preferred_element_type=f32).astype(bf)
            for t in range(2):
                g[gl, 4 * (q // 2) + lax.rem(q, 2), t] = gu[:, t * d2:(t + 1) * d2]
                g[gl, 4 * (q // 2) + 2 + t, lax.rem(q, 2)] = gd[:, t * d2:(t + 1) * d2]
            c_state[...] += lax.dot_general(pre, wu, NT, preferred_element_type=f32)
        @pl.when(step == layers)
        def _():
            for r in range(2):
                xs = x[:, pl.ds(pl.multiple_of((2 * q + r) * tr, tr), tr)]
                gi = lax.dot_general(xs, c_low[...], TN, preferred_element_type=f32).astype(bf)
                for t in range(2):
                    g[gl, 2 * q + t, r] = gi[:, t * d2:(t + 1) * d2]
    def block(b, _):
        lax.fori_loop(2 * b - 4, 2 * b - 2, tick, 0)
        chunk(b // 4, lax.rem(b, 4))
        return 0
    lax.fori_loop(0, 2 + (nu + o8 + 1) // 2, block, 0)

def gradient_sum(scale, x, y, w_in, w_up, w_down, part, kinds, types, lags=(1, 2, {"mid": 2, "late": 2, "early": 4}, 1), cid=0, K=8, KZ=8, NS=16, NF=32):
    layers, d, ff = w_up.shape
    rows = x.shape[0]
    nu, tr, tw = 8 * (layers + 1), 512, d // 2
    l0, lp, lz, ld = lags
    vm = pl.BlockSpec(memory_space=pltpu.VMEM)
    hb = pl.BlockSpec(memory_space=pl.ANY)
    sem = pltpu.SemaphoreType.DMA
    hops = plan(types, tr, tw, K, KZ)
    left = jax.ShapeDtypeStruct((max(part, 8), tr // 4, tw), bf)
    return pl.pallas_call(
        functools.partial(grad_sum_kernel, layers, scale, nu, part, tr, tw, lags, kinds, [n for n, _ in hops]),
        out_shape=[jax.ShapeDtypeStruct((nu - part, 2, tr, tw), bf)] + [left] * 4,
        in_specs=[hb, vm, hb, hb, hb],
        out_specs=[hb] * 5,
        scratch_shapes=[pltpu.VMEM(x.shape, bf), pltpu.VMEM((layers, rows, d), bf), pltpu.VMEM((rows, d), f32), pltpu.VMEM((rows, d), bf),
                        pltpu.VMEM((2, d, ff), f32), pltpu.VMEM((2, ff, d), f32), sem((2, 2)), sem((5,)), pltpu.VMEM((2, 8, 2, tr, tw), bf),
                        pltpu.VMEM((NS, tr, tw), bf), pltpu.VMEM((NF, tr, tw), bf), pltpu.VMEM((K, tr, tw), bf)]
        + [sem((K,))] * 5 + [sem((2, K))] * 3 + [spec for _, spec in hops],
        compiler_params=pltpu.CompilerParams(collective_id=cid, has_side_effects=True, vmem_limit_bytes=63 * 2**20),
        name="gradient_sum",
    )(x, y, w_in, w_up, w_down)


SLOTS, GRANTS = (4, 3, 3), (56, 44, 43)
def upd_kernel(layers, lo, hi, eta, mu, *refs):
    scratch = refs[-11:]
    wu, mu_, wd, md, g, h, p, a, ld_s, st_s, g_s = scratch
    first, last = lo == 0, hi == layers
    slots = wu.shape[0]
    if first:
        x_hbm, gs, w_in, w_up, w_dn, m_in, m_up, m_dn, nw_in, nw_up, nw_dn, nm_in, nm_up, nm_dn, h_out, x, x_s = refs[:-11]
    elif last:
        y, h_in, *pieces = refs[:10]
        w_up, w_dn, m_up, m_dn, _, _, _, _, nw_up, nw_dn, nm_up, nm_dn, loss, h_out = refs[10:-11]
    else:
        h_in, gs, w_up, w_dn, m_up, m_dn, _, _, _, _, nw_up, nw_dn, nm_up, nm_dn, h_out = refs[:-11]
    d, ff = w_up.shape[1:]
    d2, hf = d // 2, ff // 2
    ins = 4 if first else 0
    steps = ins + 2 * (hi - lo)
    def where(s):
        v = jnp.maximum(s - ins, 0)
        return lo + v // 2, lax.rem(v, 2)
    def moves(s, group, put):
        sl = lax.rem(s, slots)
        if group == "in":
            at = pl.ds(pl.multiple_of(s * hf, hf), hf)
            arr = [((w_in, nw_in)[put].at[at], wd.at[sl]), ((m_in, nm_in)[put].at[at], md.at[sl])]
        else:
            l, j = where(s)
            at = pl.ds(pl.multiple_of(j * hf, hf), hf)
            if group == "up":
                arr = [((w_up, nw_up)[put].at[l, :, at], wu.at[sl]), ((m_up, nm_up)[put].at[l, :, at], mu_.at[sl])]
            else:
                arr = [((w_dn, nw_dn)[put].at[l, at], wd.at[sl]), ((m_dn, nm_dn)[put].at[l, at], md.at[sl])]
        o = 0 if group == "up" else 2
        sems = (ld_s, st_s)[put]
        return [pltpu.make_async_copy(*((v, hb) if put else (hb, v)), sems.at[sl, o + i]) for i, (hb, v) in enumerate(arr)]
    def grads(s, kind, what):
        sl = lax.rem(s, slots)
        if kind == "in":
            c = pltpu.make_async_copy(gs.at[pl.ds(2 * s, 2)], g.at[sl, pl.ds(0, 2)], g_s.at[sl, 0])
            return getattr(c, what)()
        l, j = where(s)
        if not last:
            c = pltpu.make_async_copy(gs.at[pl.ds(8 + 8 * l + 4 * j, 4)], g.at[sl], g_s.at[sl, 0])
            return getattr(c, what)()
        me = lax.axis_index("data")
        c, q = lax.rem(me, 2), 128
        at = 8 * (l - lo) + 4 * j
        for k in range(2):
            b = lax.rem(me // (2, 4)[k], 2)
            for i in range(4):
                row = pl.multiple_of(256 * k + q * (b if i < 2 else 1 - b), q)
                half = c if i % 2 == 0 else 1 - c
                if i < 2:
                    cp = pltpu.make_async_copy(pieces[4 * k + i].at[pl.ds(at, 4)], g.at[sl, :, half, pl.ds(row, q)], g_s.at[sl, 4 * k + i])
                    getattr(cp, what)()
                elif what == "wait":
                    for u in range(4):
                        g[sl, u, half, pl.ds(row, q)] = pieces[4 * k + i][at + u]
    def on(s, kind, f):
        if kind == "in":
            if first: pl.when(jnp.logical_and(s >= 0, s < ins))(f)
        else:
            pl.when(jnp.logical_and(s >= ins, s < steps))(f)
    def load(s):
        def go_in():
            grads(s, "in", "start")
            for c in moves(s, "in", 0): c.start()
        def go():
            grads(s, "layer", "start")
            for c in moves(s, "up", 0) + moves(s, "down", 0): c.start()
        on(s, "in", go_in); on(s, "layer", go)
    def stored(s):
        def go_in():
            for c in moves(s, "in", 1): c.wait()
        def go():
            for c in moves(s, "up", 1) + moves(s, "down", 1): c.wait()
        on(s, "in", go_in); on(s, "layer", go)
    if first:
        cp_x = pltpu.make_async_copy(x_hbm, x, x_s.at[0])
        cp_x.start()
    for s in range(slots - 1): load(jnp.int32(s))
    if first: cp_x.wait()
    h[...] = jnp.zeros_like(h) if first else h_in[...]
    def step(s, _):
        sl = lax.rem(s, slots)
        def upd(w, m, u, t, ix):
            nm = mu * m[(sl, *ix)] + g[sl, u, t].astype(f32)
            m[(sl, *ix)] = nm
            nw = w[(sl, *ix)] - eta * nm
            w[(sl, *ix)] = nw
            return nw.astype(bf)
        def down(lhs, u0):
            for j in range(2):
                cols = slice(j * d2, (j + 1) * d2)
                tot = h[:, cols]
                for t in range(2):
                    r = slice(t * hf // 2, (t + 1) * hf // 2)
                    tot = tot + dot(lhs(r), upd(wd, md, u0 + j, t, (r, cols)))
                h[:, cols] = tot
        def do_in():
            grads(s, "in", "wait")
            for c in moves(s, "in", 0): c.wait()
            xs = x[:, pl.ds(pl.multiple_of(s * hf, hf), hf)]
            down(lambda r: xs[:, r], 0)
            for c in moves(s, "in", 1): c.start()
        def do_layer():
            grads(s, "layer", "wait")
            for c in moves(s, "up", 0): c.wait()
            @pl.when(where(s)[1] == 0)
            def _(): p[...] = h[...].astype(bf)
            for j in range(2):
                for t in range(2):
                    cols = slice(hf // 2 * j + d2 * t, hf // 2 * j + d2 * (t + 1))
                    a[:, cols] = gelu_tanh(dot(p[...], upd(wu, mu_, j, t, (slice(None), cols)))).astype(bf)
            for c in moves(s, "up", 1): c.start()
            for c in moves(s, "down", 0): c.wait()
            down(lambda r: a[:, r], 2)
            for c in moves(s, "down", 1): c.start()
        on(s, "in", do_in); on(s, "layer", do_layer)
        stored(s - 1)
        load(s + slots - 1)
        return 0
    lax.fori_loop(0, steps, step, 0)
    h_out[...] = h[...]
    if last:
        e = h[...] - y[...].astype(f32)
        loss[...] = jnp.sum(e * e, axis=1) / (2 * d)
    stored(jnp.int32(steps - 1))

def flip(v, mask, n):
    return lax.ppermute(v, "data", [(i, i ^ mask) for i in range(n)])

def update(eta, mu, x, y, g, halves, w_in, w_up, w_down, m_in, m_up, m_down, n):
    rows = x.shape[0]
    layers, d, ff = w_up.shape
    own_a, own_b, oth_a, oth_b = halves
    mid = layers - own_a.shape[0] // 8
    vm = pl.BlockSpec(memory_space=pltpu.VMEM)
    hb = pl.BlockSpec(memory_space=pl.ANY)
    sem = pltpu.SemaphoreType.DMA
    def scratch(slots, first):
        own_x = [pltpu.VMEM(x.shape, bf), sem((1,))] if first else []
        return own_x + [pltpu.VMEM((slots, d, ff // 2), f32)] * 2 + [pltpu.VMEM((slots, ff // 2, d), f32)] * 2 + [
            pltpu.VMEM((slots, 4, 2, 512, d // 2), bf), pltpu.VMEM((rows, d), f32), pltpu.VMEM((rows, d), bf),
            pltpu.VMEM((rows, ff // 2), bf), sem((slots, 4)), sem((slots, 4)), sem((slots, 8))]
    h_type = jax.ShapeDtypeStruct((rows, d), f32)
    def call(lo, hi, outs, ins, specs, aliases):
        which = 0 if lo == 0 else 2 if hi == layers else 1
        c = (8 * (hi - lo) + 8 * (lo == 0)) * 512 * d
        return pl.pallas_call(
            functools.partial(upd_kernel, layers, lo, hi, eta, mu), out_shape=outs, in_specs=specs,
            out_specs=[hb if len(t.shape) > 2 or t.shape[0] > rows else vm for t in outs], scratch_shapes=scratch(SLOTS[which], lo == 0),
            compiler_params=pltpu.CompilerParams(vmem_limit_bytes=GRANTS[which] * 2**20),
            input_output_aliases=aliases, cost_estimate=pl.CostEstimate(flops=4 * rows * c, bytes_accessed=18 * c, transcendentals=0),
            name="update_" + str(lo),
        )(*ins)
    o = [jax.ShapeDtypeStruct(t.shape, f32) for t in (w_in, w_up, w_down, m_in, m_up, m_down)]
    cut = mid - 1
    ax, bx = flip(own_a, 2, n), flip(own_b, 4, n)
    nw_in, nw_up, nw_dn, nm_in, nm_up, nm_dn, h = call(
        0, cut, o + [h_type], (x, g, w_in, w_up, w_down, m_in, m_up, m_down), [hb] * 8, {})
    h, ax, bx = lax.optimization_barrier((h, ax, bx))
    ac, bc = flip(ax, 1, n), flip(bx, 1, n)
    mats = [o[1], o[2], o[4], o[5]]
    nw_up, nw_dn, nm_up, nm_dn, h = call(
        cut, mid, mats + [h_type], (h, g, w_up, w_down, m_up, m_down, nw_up, nw_dn, nm_up, nm_dn), [vm] + [hb] * 9,
        {6: 0, 7: 1, 8: 2, 9: 3})
    nw_up, nw_dn, nm_up, nm_dn, loss, h = call(
        mid, layers, mats + [jax.ShapeDtypeStruct((rows,), f32), h_type],
        (y, h, own_a, oth_a, ax, ac, own_b, oth_b, bx, bc, w_up, w_down, m_up, m_down, nw_up, nw_dn, nm_up, nm_dn), [vm] * 2 + [hb, hb, vm, vm] * 2 + [hb] * 8,
        {14: 0, 15: 1, 16: 2, 17: 3})
    return nw_in, nw_up, nw_dn, nm_in, nm_up, nm_dn, loss, h

PERMUTED_LAYERS = 6

def solution(mesh):
    group_size = mesh.shape["data"]

    def device_steps(w_in, w_up, w_down, mom_in, mom_up, mom_down, x_now, y_now, x_next, y_next):
        local_rows, model_width = y_now.shape
        step_size = 4.0 * model_width / (w_up.shape[2] * (w_up.shape[0] + 1))
        part = 8 * PERMUTED_LAYERS
        def kinds(u, ty):
            odd = lax.rem(u, 2) == 1
            if ty == "late":
                return jnp.logical_and(u < part, odd)
            return jnp.logical_or(u >= part, jnp.logical_not(odd))
        total, own_a, own_b, oth_a, oth_b = gradient_sum(
            float(local_rows * group_size * model_width), x_now, y_now, w_in, w_up, w_down, part, kinds, ("late", "mid"))
        return update(step_size, MOMENTUM, x_next, y_next, total, (own_a, own_b, oth_a, oth_b), w_in, w_up, w_down, mom_in, mom_up, mom_down, group_size)

    row_spec = P("data", None)
    return jax.shard_map(
        device_steps,
        mesh=mesh,
        in_specs=(P(),) * 6 + (row_spec,) * 4,
        out_specs=(P(),) * 6 + (P("data"), row_spec),
        check_vma=False,
    )
```

```python
import functools

import jax
import jax.numpy as jnp
from jax import lax
from jax.experimental import pallas as pl
from jax.experimental.pallas import tpu as pltpu
from jax.sharding import PartitionSpec as P

MOMENTUM = 0.9
MESH = pl.DeviceIdType.MESH
BIT = {"c": 1, "x": 2, "y": 4, "a": 8, "b": 16}

bf, f32 = jnp.bfloat16, jnp.float32
TN = (((0,), (0,)), ((), ()))
NT = (((1,), (1,)), ((), ()))
def dot(a, b): return jnp.dot(a, b, preferred_element_type=f32)
def gelu_tanh(v): return jax.nn.gelu(v, approximate=True)

HOPS = {"mid": (0, "z", 1), "late": (0, 1, "z"), "early": ("z", 0, 1)}

def plan(types, tr, tw, K, KZ):
    sem, out = pltpu.SemaphoreType.DMA, []
    for ty in types:
        size = tr // 2
        for s, hop in enumerate(HOPS[ty]):
            if hop == "z":
                size //= 4
                out += [((ty, s, b), pltpu.VMEM((2, KZ, 3 * size, tw), bf)) for b in ("up", "down")]
                out += [((ty, s, b), sem((2, 2, KZ))) for b in ("rs", "rr", "as", "ar")]
            else:
                size //= 2
                out += [((ty, s, "buf"), pltpu.VMEM((2, K, size, tw), bf))]
                out += [((ty, s, b), sem((2, K))) for b in ("rs", "rr", "as", "ar")]
    return out

def grad_sum_kernel(layers, scale, nu, part, tr, tw, lags, kinds, names, *refs):
    (x_hbm, y, w_in, w_up, w_dn, gs, own_a, own_b, oth_a, oth_b, x, p_all, c_state, c_low, wup, wdn, w_s, x_s, g, acc, fin, rb0,
     c_s, c_r, d_s, d_r, st_s, h_s, h_r, hs_s) = refs[:30]
    mem = dict(zip(names, refs[30:]))
    types = sorted({n[0] for n in names})
    K, NS, NF = c_s.shape[0], acc.shape[0], fin.shape[0]
    KZ = [mem[n].shape[1] for n in names if n[2] == "up"][0]
    l0, lp, lz, ld = lags
    me = lax.axis_index("data")
    bit = {"c": lax.rem(me, 2), "x": lax.rem(me // 2, 2), "y": lax.rem(me // 4, 2)}
    peer = {d: me + w * (1 - 2 * bit[d]) for d, w in (("c", 1), ("x", 2), ("y", 4))}
    z = me // 8
    bar = pltpu.get_barrier_semaphore()
    def greet(dev):
        pl.semaphore_signal(bar, inc=1, device_id=(dev,), device_id_type=MESH)
    for d in "cxy":
        greet(peer[d])
    pl.when(z < 3)(lambda: greet(me + 8))
    pl.when(z > 0)(lambda: greet(me - 8))
    half, big = tr // 2, tr // 4
    DIMS = ("xy", "yx")
    o1 = l0
    def offsets(ty):
        zl = lz[ty]
        o4 = o1 + 2 * lp + 3 * zl
        o7 = 2 * o4 - o1
        return zl, o4, o7, o7 + ld
    o8 = max(offsets(ty)[3] for ty in types)
    assert NS >= max(offsets(ty)[1] for ty in types) and NF >= o8 - o1
    def rows(off, n):
        return pl.ds(pl.multiple_of(off, 16), n)
    def remote(src, dst, ss, rs, dev):
        return pltpu.make_async_remote_copy(src_ref=src, dst_ref=dst, send_sem=ss, recv_sem=rs, device_id=(dev,), device_id_type=MESH)
    def ix(u): return lax.rem(u, K)
    def iz(u): return lax.rem(u, KZ)
    def accr(u, off, n): return acc.at[lax.rem(u, NS), rows(off, n)]
    def finr(u, off, n): return fin.at[lax.rem(u, NF), rows(off, n)]
    def own(u): return lax.rem(u // 8, 2), lax.rem(u, 8)
    def out(u): return nu - 8 - 8 * (u // 8) + lax.rem(u, 8)
    def out_p(u): return part - 8 - 8 * (u // 8) + lax.rem(u, 8)
    def cp_c(u):
        return remote(g.at[(*own(u), 1 - bit["c"])], rb0.at[ix(u)], c_s.at[ix(u)], c_r.at[ix(u)], peer["c"])
    def cp_d(u):
        return remote(fin.at[lax.rem(u, NF)], gs.at[out(u), bit["c"]], d_s.at[ix(u)], d_r.at[ix(u)], peer["c"])
    def cp_st(u):
        return pltpu.make_async_copy(fin.at[lax.rem(u, NF)], gs.at[out(u), bit["c"]], st_s.at[ix(u)])
    home = [k * half + big * bit[DIMS[k][0]] for k in range(2)]
    def cp_h(u, k):
        return remote(finr(u, home[k], big), (oth_a, oth_b)[k].at[out_p(u)], h_s.at[k, ix(u)], h_r.at[k, ix(u)], peer["c"])
    def cp_hs(u, k):
        return pltpu.make_async_copy(finr(u, home[k], big), (own_a, own_b)[k].at[out_p(u)], hs_s.at[k, ix(u)])
    def add(dst, slot, r, a, b):
        dst[slot, r] = (a.astype(f32) + b.astype(f32)).astype(bf)
    snd_r = [lambda q: (q + 1, 3 - q), lambda q: (0, q)]
    rcv_r = [lambda q: (q, 4 - q), lambda q: (0, q + 1)]
    snd_a = [lambda q: (0, q + 1), lambda q: (q, 4 - q)]
    rcv_a = [lambda q: (0, q), lambda q: (q + 1, 3 - q)]
    senders, takers = [(0, 1, 2), (1, 2, 3)], [(1, 2, 3), (0, 1, 2)]
    def tick(t, _):
        def ev(off, f, cond=None):
            u = t - off
            ok = jnp.logical_and(u >= 0, u < nu)
            if cond is not None: ok = jnp.logical_and(ok, cond(u))
            pl.when(ok)(lambda: f(u))
        def whole(u): return u >= part
        def left(u): return u < part
        def e8(u):
            cp_d(u).wait(); cp_st(u).wait()
        def e8p(u):
            for k in range(2):
                cp_h(u, k).wait(); cp_hs(u, k).wait()
        def e7(u):
            cp_d(u).start(); cp_st(u).start()
        def e6p(u):
            for k in range(2):
                cp_h(u, k).start(); cp_hs(u, k).start()
        def e1(u):
            cp_c(u).wait()
            so, uo = own(u)
            for q in range(4):
                r = slice(q * big, (q + 1) * big)
                add(acc, lax.rem(u, NS), r, g[so, uo, bit["c"], r], rb0[ix(u), r])
        def line(ty, s, base, ch, o, lz, cond, gather, what):
            bufs, names_ = (mem[ty, s, "up"], mem[ty, s, "down"]), ("as", "ar") if gather else ("rs", "rr")
            snd, rcv = (snd_a, rcv_a) if gather else (snd_r, rcv_r)
            at = [o + z * lz, o + (3 - z) * lz]
            def cp(u, k, side, f, n):
                ss, rs = (mem[ty, s, m].at[side, k, iz(u)] for m in names_)
                r = (finr if gather else accr)(u, base[k] + ch * f, n * ch)
                return remote(r, r if gather else bufs[side].at[k, iz(u), pl.ds(0, n * ch)], ss, rs, me + (8, -8)[side])
            for side in range(2):
                if what == "arrive":
                    for q in senders[side]:
                        def sent(u, side=side, q=q):
                            for k in range(2): cp(u, k, side, *snd[side](q)).wait_send()
                        pl.when(z == q)(lambda: ev(at[side] + lz, sent, cond))
                    for q in takers[side]:
                        def got(u, side=side, q=q):
                            f, n = rcv[side](q)
                            for k in range(2):
                                cp(u, k, side, f, n).wait_recv()
                                if not gather:
                                    r = rows(base[k] + ch * f, n * ch)
                                    add(acc, lax.rem(u, NS), r, acc[lax.rem(u, NS), r], bufs[side][k, iz(u), 0:n * ch])
                        pl.when(z == q)(lambda: ev(at[side], got, cond))
                else:
                    for q in senders[side]:
                        def send(u, side=side, q=q):
                            for k in range(2): cp(u, k, side, *snd[side](q)).start()
                        pl.when(z == q)(lambda: ev(at[side], send, cond))
        def flow(ty):
            zl, o4, o7, o8 = offsets(ty)
            mine = lambda u: kinds(u, ty)
            mine_whole = lambda u: jnp.logical_and(mine(u), whole(u))
            ev(o8, e8, mine_whole)
            if part: ev(o7, e8p, lambda u: jnp.logical_and(mine(u), left(u)))
            base, size, hops = [[0, half]], [half], []
            o = o1
            for s, hop in enumerate(HOPS[ty]):
                if hop == "z":
                    n = size[-1] // 4
                    nb = [b + n * z for b in base[-1]]
                    give, dim = None, None
                    lag = 3 * zl
                else:
                    n = size[-1] // 2
                    dim = [DIMS[k][hop] for k in range(2)]
                    nb = [base[-1][k] + n * bit[dim[k]] for k in range(2)]
                    give = [base[-1][k] + n * (1 - bit[dim[k]]) for k in range(2)]
                    lag = lp
                hops.append((s, hop, base[-1], nb, n, give, dim, o, o + lag))
                base.append(nb); size.append(n)
                o += lag
            last_base, last = base[-1], size[-1]
            def pair_cp(u, k, s, src, dst, pre, dev):
                return remote(src, dst, mem[ty, s, pre + "s"].at[k, ix(u)], mem[ty, s, pre + "r"].at[k, ix(u)], peer[dev])
            o = o7
            for i, (s, hop, b, nb, n, give, dim, _, _) in enumerate(hops):
                cond = mine_whole if i == 0 else mine
                if hop == "z":
                    line(ty, s, b, n, o - 3 * zl, zl, cond, True, "arrive")
                else:
                    def arrive(u, s=s, nb=nb, n=n, dim=dim):
                        for k in range(2): pair_cp(u, k, s, finr(u, nb[k], n), finr(u, nb[k], n), "a", dim[k]).wait()
                    ev(o, arrive, cond)
                if i == 0:
                    ev(o7, e7, mine_whole)
                else:
                    depart_g(*prev)
                    if i == 1 and part: ev(o, e6p, lambda u: jnp.logical_and(mine(u), left(u)))
                def depart_g(s, hop, b, nb, n, dim, o, cond):
                    if hop == "z":
                        line(ty, s, b, n, o, zl, cond, True, "depart")
                    else:
                        def go(u):
                            for k in range(2): pair_cp(u, k, s, finr(u, nb[k], n), finr(u, nb[k], n), "a", dim[k]).start()
                        ev(o, go, cond)
                o -= 3 * zl if hop == "z" else lp
                prev = (s, hop, b, nb, n, dim, o, cond)
            for i, (s, hop, b, nb, n, give, dim, oa, ob) in reversed(list(enumerate(hops))):
                if hop == "z":
                    line(ty, s, b, n, oa, zl, mine, False, "arrive")
                else:
                    def arrive(u, s=s, nb=nb, n=n, give=give, dim=dim):
                        for k in range(2):
                            pair_cp(u, k, s, accr(u, give[k], n), mem[ty, s, "buf"].at[k, ix(u)], "r", dim[k]).wait()
                            r = rows(nb[k], n)
                            add(acc, lax.rem(u, NS), r, acc[lax.rem(u, NS), r], mem[ty, s, "buf"][k, ix(u)])
                    ev(ob, arrive, mine)
                if i == len(hops) - 1:
                    def finish(u):
                        for k in range(2):
                            r = rows(last_base[k], last)
                            fin[lax.rem(u, NF), r] = acc[lax.rem(u, NS), r]
                    ev(o4, finish, mine)
                    depart_g(*prev)
                else:
                    depart_r(*prev_r)
                def depart_r(s, hop, b, n, give, dim, oa):
                    if hop == "z":
                        line(ty, s, b, n, oa, zl, mine, False, "depart")
                    else:
                        def go(u):
                            for k in range(2): pair_cp(u, k, s, accr(u, give[k], n), mem[ty, s, "buf"].at[k, ix(u)], "r", dim[k]).start()
                        ev(oa, go, mine)
                prev_r = (s, hop, b, n, give, dim, oa)
            return depart_r, prev_r
        firsts = [flow(ty) for ty in types]
        ev(o1, e1)
        for f, args in firsts: f(*args)
        ev(0, lambda u: cp_c(u).start())
        return 0
    d, ff = w_up.shape[1:]
    def cp_w(layer, k):
        sl = lax.rem(layer, 2)
        src, dst = ((w_up, wup), (w_dn, wdn))[k]
        return pltpu.make_async_copy(src.at[layer], dst.at[sl], w_s.at[k, sl])
    e4 = w_in.shape[0] // 4
    cp_x = pltpu.make_async_copy(x_hbm, x, x_s.at[4])
    cp_in = [pltpu.make_async_copy(w_in.at[pl.ds(i * e4, e4)], wdn.at[i // 2, pl.ds((i % 2) * e4, e4)], x_s.at[i]) for i in range(4)]
    cp_x.start()
    for c in cp_in: c.start()
    for l in range(2): cp_w(l, 0).start()
    cp_x.wait()
    h = c_state
    for i in range(4):
        cp_in[i].wait()
        piece = dot(x[:, i * e4:(i + 1) * e4], wdn[i // 2, (i % 2) * e4:(i % 2 + 1) * e4].astype(bf))
        h[...] = piece if i == 0 else h[...] + piece
        if i % 2 == 1: cp_w(i // 2, 1).start()
    n = ff // 4
    def layer_fwd(l, _):
        sl = lax.rem(l, 2)
        pin = h[...].astype(bf)
        p_all[l] = pin
        tot = h[...]
        cp_w(l, 0).wait()
        acts = [gelu_tanh(dot(pin, wup[sl, :, q * n:(q + 1) * n].astype(bf))).astype(bf) for q in range(4)]
        cp_w(l, 1).wait()
        for q in range(4):
            tot = tot + dot(acts[q], wdn[sl, q * n:(q + 1) * n].astype(bf))
        h[...] = tot
        @pl.when(l < layers - 2)
        def _():
            for k in range(2): cp_w(l + 2, k).start()
        return 0
    lax.fori_loop(0, layers, layer_fwd, 0)
    c_state[...] = (h[...] - y[...].astype(f32)) / scale
    pl.semaphore_wait(bar, 3 + jnp.minimum(z, 1) + jnp.minimum(3 - z, 1))
    d2 = d // 2
    def chunk(step, q):
        gl = lax.rem(step, 2)
        layer = layers - 1 - step
        sl = lax.rem(layer, 2)
        @pl.when(jnp.logical_and(q == 0, step <= layers))
        def _():
            c_low[...] = c_state[...].astype(bf)
        @pl.when(jnp.logical_and(q == 0, jnp.logical_and(step >= 2, step < layers)))
        def _():
            for k in range(2): cp_w(layer, k).wait()
        @pl.when(jnp.logical_and(q == 0, jnp.logical_and(step >= 1, step < layers - 1)))
        def _():
            for k in range(2): cp_w(layer - 1, k).start()
        @pl.when(step < layers)
        def _():
            cols = pl.ds(pl.multiple_of(q * n, n), n)
            pin = p_all[layer]
            wu = wup[sl, :, cols].astype(bf)
            act, back = jax.vjp(gelu_tanh, dot(pin, wu))
            ac = lax.dot_general(c_low[...], wdn[sl, cols, :].astype(bf), NT, preferred_element_type=f32)
            pre = back(ac)[0].astype(bf)
            gd = lax.dot_general(act.astype(bf), c_low[...], TN, preferred_element_type=f32).astype(bf)
            gu = lax.dot_general(pin, pre, TN, preferred_element_type=f32).astype(bf)
            for t in range(2):
                g[gl, 4 * (q // 2) + lax.rem(q, 2), t] = gu[:, t * d2:(t + 1) * d2]
                g[gl, 4 * (q // 2) + 2 + t, lax.rem(q, 2)] = gd[:, t * d2:(t + 1) * d2]
            c_state[...] += lax.dot_general(pre, wu, NT, preferred_element_type=f32)
        @pl.when(step == layers)
        def _():
            for r in range(2):
                xs = x[:, pl.ds(pl.multiple_of((2 * q + r) * tr, tr), tr)]
                gi = lax.dot_general(xs, c_low[...], TN, preferred_element_type=f32).astype(bf)
                for t in range(2):
                    g[gl, 2 * q + t, r] = gi[:, t * d2:(t + 1) * d2]
    def block(b, _):
        lax.fori_loop(2 * b - 4, 2 * b - 2, tick, 0)
        chunk(b // 4, lax.rem(b, 4))
        return 0
    lax.fori_loop(0, 2 + (nu + o8 + 1) // 2, block, 0)

def gradient_sum(scale, x, y, w_in, w_up, w_down, part, kinds, types, lags=(1, 2, {"mid": 2, "late": 2, "early": 4}, 1), cid=0, K=8, KZ=8, NS=16, NF=32):
    layers, d, ff = w_up.shape
    rows = x.shape[0]
    nu, tr, tw = 8 * (layers + 1), 512, d // 2
    l0, lp, lz, ld = lags
    vm = pl.BlockSpec(memory_space=pltpu.VMEM)
    hb = pl.BlockSpec(memory_space=pl.ANY)
    sem = pltpu.SemaphoreType.DMA
    hops = plan(types, tr, tw, K, KZ)
    left = jax.ShapeDtypeStruct((max(part, 8), tr // 4, tw), bf)
    return pl.pallas_call(
        functools.partial(grad_sum_kernel, layers, scale, nu, part, tr, tw, lags, kinds, [n for n, _ in hops]),
        out_shape=[jax.ShapeDtypeStruct((nu - part, 2, tr, tw), bf)] + [left] * 4,
        in_specs=[hb, vm, hb, hb, hb],
        out_specs=[hb] * 5,
        scratch_shapes=[pltpu.VMEM(x.shape, bf), pltpu.VMEM((layers, rows, d), bf), pltpu.VMEM((rows, d), f32), pltpu.VMEM((rows, d), bf),
                        pltpu.VMEM((2, d, ff), f32), pltpu.VMEM((2, ff, d), f32), sem((2, 2)), sem((5,)), pltpu.VMEM((2, 8, 2, tr, tw), bf),
                        pltpu.VMEM((NS, tr, tw), bf), pltpu.VMEM((NF, tr, tw), bf), pltpu.VMEM((K, tr, tw), bf)]
        + [sem((K,))] * 5 + [sem((2, K))] * 3 + [spec for _, spec in hops],
        compiler_params=pltpu.CompilerParams(collective_id=cid, has_side_effects=True, vmem_limit_bytes=63 * 2**20),
        name="gradient_sum",
    )(x, y, w_in, w_up, w_down)


SLOTS, GRANTS = (4, 3, 3), (52, 44, 43)
def upd_kernel(layers, lo, hi, eta, mu, *refs):
    scratch = refs[-11:]
    wu, mu_, wd, md, g, h, p, a, ld_s, st_s, g_s = scratch
    first, last = lo == 0, hi == layers
    slots = wu.shape[0]
    if first:
        x_hbm, gs, w_in, w_up, w_dn, m_in, m_up, m_dn, nw_in, nw_up, nw_dn, nm_in, nm_up, nm_dn, h_out, x, x_s = refs[:-11]
    elif last:
        y, h_in, *pieces = refs[:10]
        w_up, w_dn, m_up, m_dn, _, _, _, _, nw_up, nw_dn, nm_up, nm_dn, loss, h_out = refs[10:-11]
    else:
        h_in, gs, w_up, w_dn, m_up, m_dn, _, _, _, _, nw_up, nw_dn, nm_up, nm_dn, h_out = refs[:-11]
    d, ff = w_up.shape[1:]
    d2, hf = d // 2, ff // 2
    ins = 4 if first else 0
    steps = ins + 2 * (hi - lo)
    def where(s):
        v = jnp.maximum(s - ins, 0)
        return lo + v // 2, lax.rem(v, 2)
    def moves(s, group, put):
        sl = lax.rem(s, slots)
        if group == "in":
            at = pl.ds(pl.multiple_of(s * hf, hf), hf)
            arr = [((w_in, nw_in)[put].at[at], wd.at[sl]), ((m_in, nm_in)[put].at[at], md.at[sl])]
        else:
            l, j = where(s)
            at = pl.ds(pl.multiple_of(j * hf, hf), hf)
            if group == "up":
                arr = [((w_up, nw_up)[put].at[l, :, at], wu.at[sl]), ((m_up, nm_up)[put].at[l, :, at], mu_.at[sl])]
            else:
                arr = [((w_dn, nw_dn)[put].at[l, at], wd.at[sl]), ((m_dn, nm_dn)[put].at[l, at], md.at[sl])]
        o = 0 if group == "up" else 2
        sems = (ld_s, st_s)[put]
        return [pltpu.make_async_copy(*((v, hb) if put else (hb, v)), sems.at[sl, o + i]) for i, (hb, v) in enumerate(arr)]
    def grads(s, kind, what):
        sl = lax.rem(s, slots)
        if kind == "in":
            c = pltpu.make_async_copy(gs.at[pl.ds(2 * s, 2)], g.at[sl, pl.ds(0, 2)], g_s.at[sl, 0])
            return getattr(c, what)()
        l, j = where(s)
        if not last:
            c = pltpu.make_async_copy(gs.at[pl.ds(8 + 8 * l + 4 * j, 4)], g.at[sl], g_s.at[sl, 0])
            return getattr(c, what)()
        me = lax.axis_index("data")
        c, q = lax.rem(me, 2), 128
        at = 8 * (l - lo) + 4 * j
        for k in range(2):
            b = lax.rem(me // (2, 4)[k], 2)
            for i in range(4):
                row = pl.multiple_of(256 * k + q * (b if i < 2 else 1 - b), q)
                half = c if i % 2 == 0 else 1 - c
                if i < 2:
                    cp = pltpu.make_async_copy(pieces[4 * k + i].at[pl.ds(at, 4)], g.at[sl, :, half, pl.ds(row, q)], g_s.at[sl, 4 * k + i])
                    getattr(cp, what)()
                elif what == "wait":
                    for u in range(4):
                        g[sl, u, half, pl.ds(row, q)] = pieces[4 * k + i][at + u]
    def on(s, kind, f):
        if kind == "in":
            if first: pl.when(jnp.logical_and(s >= 0, s < ins))(f)
        else:
            pl.when(jnp.logical_and(s >= ins, s < steps))(f)
    def load(s):
        def go_in():
            grads(s, "in", "start")
            for c in moves(s, "in", 0): c.start()
        def go():
            grads(s, "layer", "start")
            for c in moves(s, "up", 0) + moves(s, "down", 0): c.start()
        on(s, "in", go_in); on(s, "layer", go)
    def stored(s):
        def go_in():
            for c in moves(s, "in", 1): c.wait()
        def go():
            for c in moves(s, "up", 1) + moves(s, "down", 1): c.wait()
        on(s, "in", go_in); on(s, "layer", go)
    if first:
        cp_x = pltpu.make_async_copy(x_hbm, x, x_s.at[0])
        cp_x.start()
    for s in range(slots - 1): load(jnp.int32(s))
    if first: cp_x.wait()
    h[...] = jnp.zeros_like(h) if first else h_in[...]
    def step(s, _):
        sl = lax.rem(s, slots)
        def upd(w, m, u, t, ix):
            nm = mu * m[(sl, *ix)] + g[sl, u, t].astype(f32)
            m[(sl, *ix)] = nm
            nw = w[(sl, *ix)] - eta * nm
            w[(sl, *ix)] = nw
            return nw.astype(bf)
        def down(lhs, u0):
            for j in range(2):
                cols = slice(j * d2, (j + 1) * d2)
                tot = h[:, cols]
                for t in range(2):
                    r = slice(t * hf // 2, (t + 1) * hf // 2)
                    tot = tot + dot(lhs(r), upd(wd, md, u0 + j, t, (r, cols)))
                h[:, cols] = tot
        def do_in():
            grads(s, "in", "wait")
            for c in moves(s, "in", 0): c.wait()
            xs = x[:, pl.ds(pl.multiple_of(s * hf, hf), hf)]
            down(lambda r: xs[:, r], 0)
            for c in moves(s, "in", 1): c.start()
        def do_layer():
            grads(s, "layer", "wait")
            for c in moves(s, "up", 0): c.wait()
            @pl.when(where(s)[1] == 0)
            def _(): p[...] = h[...].astype(bf)
            for j in range(2):
                for t in range(2):
                    cols = slice(hf // 2 * j + d2 * t, hf // 2 * j + d2 * (t + 1))
                    a[:, cols] = gelu_tanh(dot(p[...], upd(wu, mu_, j, t, (slice(None), cols)))).astype(bf)
            for c in moves(s, "up", 1): c.start()
            for c in moves(s, "down", 0): c.wait()
            down(lambda r: a[:, r], 2)
            for c in moves(s, "down", 1): c.start()
        on(s, "in", do_in); on(s, "layer", do_layer)
        stored(s - 1)
        load(s + slots - 1)
        return 0
    lax.fori_loop(0, steps, step, 0)
    h_out[...] = h[...]
    if last:
        e = h[...] - y[...].astype(f32)
        loss[...] = jnp.sum(e * e, axis=1) / (2 * d)
    stored(jnp.int32(steps - 1))

def flip(v, mask, n):
    return lax.ppermute(v, "data", [(i, i ^ mask) for i in range(n)])

def update(eta, mu, x, y, g, halves, w_in, w_up, w_down, m_in, m_up, m_down, n):
    rows = x.shape[0]
    layers, d, ff = w_up.shape
    own_a, own_b, oth_a, oth_b = halves
    mid = layers - own_a.shape[0] // 8
    vm = pl.BlockSpec(memory_space=pltpu.VMEM)
    hb = pl.BlockSpec(memory_space=pl.ANY)
    sem = pltpu.SemaphoreType.DMA
    def scratch(slots, first):
        own_x = [pltpu.VMEM(x.shape, bf), sem((1,))] if first else []
        return own_x + [pltpu.VMEM((slots, d, ff // 2), f32)] * 2 + [pltpu.VMEM((slots, ff // 2, d), f32)] * 2 + [
            pltpu.VMEM((slots, 4, 2, 512, d // 2), bf), pltpu.VMEM((rows, d), f32), pltpu.VMEM((rows, d), bf),
            pltpu.VMEM((rows, ff // 2), bf), sem((slots, 4)), sem((slots, 4)), sem((slots, 8))]
    h_type = jax.ShapeDtypeStruct((rows, d), f32)
    def call(lo, hi, outs, ins, specs, aliases):
        which = 0 if lo == 0 else 2 if hi == layers else 1
        c = (8 * (hi - lo) + 8 * (lo == 0)) * 512 * d
        return pl.pallas_call(
            functools.partial(upd_kernel, layers, lo, hi, eta, mu), out_shape=outs, in_specs=specs,
            out_specs=[hb if len(t.shape) > 2 or t.shape[0] > rows else vm for t in outs], scratch_shapes=scratch(SLOTS[which], lo == 0),
            compiler_params=pltpu.CompilerParams(vmem_limit_bytes=GRANTS[which] * 2**20),
            input_output_aliases=aliases, cost_estimate=pl.CostEstimate(flops=4 * rows * c, bytes_accessed=18 * c, transcendentals=0),
            name="update_" + str(lo),
        )(*ins)
    o = [jax.ShapeDtypeStruct(t.shape, f32) for t in (w_in, w_up, w_down, m_in, m_up, m_down)]
    cut = mid - 1
    ax, bx = flip(own_a, 2, n), flip(own_b, 4, n)
    nw_in, nw_up, nw_dn, nm_in, nm_up, nm_dn, h = call(
        0, cut, o + [h_type], (x, g, w_in, w_up, w_down, m_in, m_up, m_down), [hb] * 8, {})
    h, ax, bx = lax.optimization_barrier((h, ax, bx))
    ac, bc = flip(ax, 1, n), flip(bx, 1, n)
    mats = [o[1], o[2], o[4], o[5]]
    nw_up, nw_dn, nm_up, nm_dn, h = call(
        cut, mid, mats + [h_type], (h, g, w_up, w_down, m_up, m_down, nw_up, nw_dn, nm_up, nm_dn), [vm] + [hb] * 9,
        {6: 0, 7: 1, 8: 2, 9: 3})
    nw_up, nw_dn, nm_up, nm_dn, loss, h = call(
        mid, layers, mats + [jax.ShapeDtypeStruct((rows,), f32), h_type],
        (y, h, own_a, oth_a, ax, ac, own_b, oth_b, bx, bc, w_up, w_down, m_up, m_down, nw_up, nw_dn, nm_up, nm_dn), [vm] * 2 + [hb, hb, vm, vm] * 2 + [hb] * 8,
        {14: 0, 15: 1, 16: 2, 17: 3})
    return nw_in, nw_up, nw_dn, nm_in, nm_up, nm_dn, loss, h

PERMUTED_LAYERS = 6

def solution(mesh):
    group_size = mesh.shape["data"]

    def device_steps(w_in, w_up, w_down, mom_in, mom_up, mom_down, x_now, y_now, x_next, y_next):
        local_rows, model_width = y_now.shape
        step_size = 4.0 * model_width / (w_up.shape[2] * (w_up.shape[0] + 1))
        part = 8 * PERMUTED_LAYERS
        def kinds(u, ty):
            odd = lax.rem(u, 2) == 1
            if ty == "late":
                return jnp.logical_and(u < part, odd)
            return jnp.logical_or(u >= part, jnp.logical_not(odd))
        total, own_a, own_b, oth_a, oth_b = gradient_sum(
            float(local_rows * group_size * model_width), x_now, y_now, w_in, w_up, w_down, part, kinds, ("late", "mid"))
        return update(step_size, MOMENTUM, x_next, y_next, total, (own_a, own_b, oth_a, oth_b), w_in, w_up, w_down, mom_in, mom_up, mom_down, group_size)

    row_spec = P("data", None)
    return jax.shard_map(
        device_steps,
        mesh=mesh,
        in_specs=(P(),) * 6 + (row_spec,) * 4,
        out_specs=(P(),) * 6 + (P("data"), row_spec),
        check_vma=False,
    )
```
